256 devices in a mesh: patch: 32 (over x, z_hi, core), tp: 8 (over y, z_lo).
Axes of the slice: x: 4, y: 4, z: 8 (z_hi: 4, z_lo: 2; z = z_hi * 2 + z_lo), core: 2. Of those that a mesh axis runs over, the one named last changes fastest.
Arguments:
- resid_corrupt: bfloat16 [512, 4096], P(None, 'tp'), may hold values from -6 to 6
- resid_clean: bfloat16 [2, 512, 4096], P(None, 'patch', 'tp'), may hold values from -6 to 6
- patch_level: int32 [32], P('patch'), may hold values from 0 to 1
- patch_mask: int32 [32, 128], P('patch'), may hold values 0 or 1
- norm_gain: bfloat16 [4096], P('tp'), may hold values from 0.099609375 to 1.8984375
- final_gain: bfloat16 [4096], P('tp'), may hold values from 0.099609375 to 1.8984375
- w_query: bfloat16 [4096, 4096], P('patch', 'tp'), may hold values from -1 to 1
- w_key: bfloat16 [4096, 1024], P('patch', 'tp'), may hold values from -1 to 1
- w_value: bfloat16 [4096, 1024], P('patch', 'tp'), may hold values from -0.09375 to 0.09375
- w_out: bfloat16 [4096, 4096], P('tp', 'patch'), may hold values from -0.09375 to 0.09375
- unembed: bfloat16 [128256, 4096], P(('patch', 'tp')), may hold values from -0.09375 to 0.09375
- scored_ids: int32 [256], replicated, may hold values from 0 to 128255
- base_logits: float32 [512, 256], P('tp'), may hold values from -6 to 6
Outputs:
- logit_shift: float32 [32, 512, 256], P('patch', 'tp')
The draws below stay inside these ranges and needn't reach their ends.
All inputs are finite; a program needn't handle non-finite values. No bound on the sum of `patch_mask` on one device may be relied on, other than what follows from the above.
Results may differ from the reference program's by a relative error of at most 0.01.
The reference program's roundings to bfloat16 on the way count: a program that leaves them out, or rounds other values in their place, can miss the bound.
Values may be sent and summed in bfloat16 or wider, within the bound.
A program may use at most 128 MiB of HBM per device.

```python
import math
import jax
import jax.numpy as jnp
from jax import lax

D = 4096
H = 32
KVH = 8
HD = 128
VOCAB = 128256
SEQ = 128
PROMPTS = 4
NSITE = 2
SCORED = 256
TOKENS = 512
GROUPS = 32
N_TP = 8


def shared_keys(key):
    return jax.random.normal(jax.random.fold_in(key, 11), (D, KVH * HD), jnp.float32)


def draw_w_query(key, part):
    own = jax.random.normal(jax.random.fold_in(key, 12), (D, H * HD), jnp.float32)
    scaled = jnp.clip(own, -6.0, 6.0) / math.sqrt(D)
    return jnp.clip(scaled, -1.0, 1.0).astype(jnp.bfloat16)


def draw_w_key(key, part):
    shared = shared_keys(key)
    scaled = jnp.clip(shared, -6.0, 6.0) / math.sqrt(D)
    return jnp.clip(scaled, -1.0, 1.0).astype(jnp.bfloat16)


def set_ends(values, own_key, smallest, top_value):
    place = [jax.random.randint(jax.random.fold_in(own_key, axis), (), 0, length) for axis, length in enumerate(values.shape)]
    widest = values.shape.index(max(values.shape))
    next_to = place[:widest] + [(place[widest] + 1) % values.shape[widest]] + place[widest + 1:]
    return values.at[tuple(place)].set(smallest).at[tuple(next_to)].set(top_value)


def block_scale(stream_key, extent, split, smallest, top_value):
    def one(dim, parts):
        steps = jax.random.uniform(jax.random.fold_in(jax.random.fold_in(stream_key, 6), dim), (parts,), jnp.float32, smallest / len(split), top_value / len(split))
        return jnp.repeat(jnp.exp(steps), extent[dim] // parts).reshape((-1,) + (1,) * (len(extent) - dim - 1))

    loudness = one(*split[0])
    for cut in split[1:]:
        loudness = loudness * one(*cut)
    return loudness


def centred(stream_key, extent, scale, limit, split=(), kind=jnp.bfloat16):
    entries = scale * jax.random.normal(stream_key, extent, jnp.float32)
    if split:
        entries = entries * block_scale(stream_key, extent, split, -0.22, 0.18)
    return jnp.clip(entries, -limit, limit).astype(kind)


def setup_inputs(seed: int = 0) -> dict:
    streams_of = jax.random.split(jax.random.key(seed), 14)
    resid_corrupt = centred(streams_of[0], (TOKENS, D), 1.0, 6.0, ((1, 8),))
    resid_clean = centred(streams_of[1], (NSITE, TOKENS, D), 1.0, 6.0, ((1, 32), (2, 8)))
    patch_level = set_ends(jax.random.randint(streams_of[2], (GROUPS,), 0, NSITE), jax.random.fold_in(streams_of[2], 1), 0, NSITE - 1).astype(jnp.int32)
    patch_mask = set_ends((jax.random.randint(streams_of[3], (GROUPS, SEQ), 0, 4) < 1).astype(jnp.int32), jax.random.fold_in(streams_of[3], 1), 0, 1)
    norm_gain = jnp.clip(1.0 + 0.18 * jax.random.normal(streams_of[4], (D,), jnp.float32), 0.099609375, 1.8984375).astype(jnp.bfloat16)
    final_gain = jnp.clip(1.0 + 0.18 * jax.random.normal(streams_of[5], (D,), jnp.float32), 0.099609375, 1.8984375).astype(jnp.bfloat16)
    w_query = draw_w_query(jax.random.fold_in(streams_of[13], 71), 0)
    w_key = draw_w_key(jax.random.fold_in(streams_of[13], 71), 0)
    w_value = centred(streams_of[8], (D, KVH * HD), D ** -0.5, 0.09375, ((0, 32), (1, 8)))
    w_out = centred(streams_of[9], (H * HD, D), (H * HD) ** -0.5, 0.09375, ((0, 8), (1, 32)))
    unembed = centred(streams_of[10], (VOCAB, D), D ** -0.5, 0.09375, ((0, 256),))
    scored_ids = set_ends(jax.random.randint(streams_of[11], (SCORED,), 0, VOCAB), jax.random.fold_in(streams_of[11], 1), 0, VOCAB - 1).astype(jnp.int32)
    base_logits = centred(streams_of[12], (TOKENS, SCORED), 1.0, 6.0, ((0, 8),), jnp.float32)
    return dict(resid_corrupt=resid_corrupt, resid_clean=resid_clean, patch_level=patch_level, patch_mask=patch_mask, norm_gain=norm_gain, final_gain=final_gain, w_query=w_query, w_key=w_key, w_value=w_value, w_out=w_out, unembed=unembed, scored_ids=scored_ids, base_logits=base_logits)


EPSILON = 1e-05
THETA = 500000.0

def rope_tables(length, head_dim):
    half = head_dim // 2
    freqs = THETA ** (-(jnp.arange(half, dtype=jnp.float32) * 2.0 / head_dim))
    angles = jnp.arange(length, dtype=jnp.float32)[:, None] * freqs[None, :]
    return (jnp.cos(angles)[:, None, :], jnp.sin(angles)[:, None, :])

def rotate(values, cosine, sine):
    half = values.shape[-1] // 2
    lower = values[..., :half]
    upper = values[..., half:]
    return jnp.concatenate([lower * cosine - upper * sine, upper * cosine + lower * sine], axis=-1)

def rms_scale(rows, gain):
    return rows * lax.rsqrt(lax.optimization_barrier(jnp.mean(rows * rows, axis=-1, keepdims=True)) + EPSILON) * gain

def one_group(level, mask_row, resid_corrupt, resid_clean, norm_gain, final_gain, w_query, w_key, w_value, w_out, score_rows, base_logits):
    row_mask = jnp.tile(mask_row, PROMPTS) == 1
    early = (row_mask & (level == 0))[:, None]
    layer_in = jnp.where(early, resid_clean[0], resid_corrupt)
    normed = rms_scale(layer_in.astype(jnp.float32), norm_gain.astype(jnp.float32)).astype(jnp.bfloat16)
    query_f = jnp.dot(normed, w_query, preferred_element_type=jnp.float32)
    key_f = jnp.dot(normed, w_key, preferred_element_type=jnp.float32)
    value_rows = jnp.dot(normed, w_value, preferred_element_type=jnp.float32).astype(jnp.bfloat16)
    cosine, sine = rope_tables(SEQ, HD)
    group = H // KVH
    queries = rotate(query_f.reshape(PROMPTS, SEQ, H, HD), cosine, sine).astype(jnp.bfloat16)
    queries = queries.reshape(PROMPTS, SEQ, KVH, group, HD)
    key_rows = rotate(key_f.reshape(PROMPTS, SEQ, KVH, HD), cosine, sine).astype(jnp.bfloat16)
    value_rows = value_rows.reshape(PROMPTS, SEQ, KVH, HD)
    scores = jnp.einsum('pqkgd,pskd->pkgqs', queries.astype(jnp.float32), key_rows.astype(jnp.float32)) * HD ** (-0.5)
    causal = jnp.arange(SEQ)[:, None] >= jnp.arange(SEQ)[None, :]
    scores = jnp.where(causal, scores, -1e+30)
    probs = jax.nn.softmax(scores, axis=-1).astype(jnp.bfloat16)
    attended = jnp.einsum('pkgqs,pskd->pqkgd', probs.astype(jnp.float32), value_rows.astype(jnp.float32))
    attended = attended.astype(jnp.bfloat16).reshape(TOKENS, H * HD)
    width = H * HD // N_TP
    head_out = jnp.zeros((TOKENS, D), jnp.float32)
    for index in range(N_TP):
        term = jnp.dot(attended[:, index * width:(index + 1) * width], w_out[index * width:(index + 1) * width], preferred_element_type=jnp.float32).astype(jnp.bfloat16)
        head_out = head_out + lax.optimization_barrier(term).astype(jnp.float32)
    middle = layer_in.astype(jnp.float32) + head_out
    late = (row_mask & (level == 1))[:, None]
    residual = jnp.where(late, resid_clean[1].astype(jnp.float32), middle)
    final_rows = rms_scale(residual, final_gain.astype(jnp.float32)).astype(jnp.bfloat16)
    logits = jnp.dot(final_rows, score_rows.T, preferred_element_type=jnp.float32)
    return logits - base_logits

def reference(resid_corrupt, resid_clean, patch_level, patch_mask, norm_gain, final_gain, w_query, w_key, w_value, w_out, unembed, scored_ids, base_logits):
    score_rows = jnp.take(unembed, scored_ids.astype(jnp.int32), axis=0)

    def step(pair):
        return one_group(pair[0], pair[1], resid_corrupt, resid_clean, norm_gain, final_gain, w_query, w_key, w_value, w_out, score_rows, base_logits)
    return lax.map(step, (patch_level, patch_mask))
```

```python
import jax
import jax.numpy as jnp
from jax import lax
from jax.experimental import pallas as pl
from jax.experimental.pallas import tpu as pltpu
from jax.sharding import PartitionSpec as P

D = 4096
HD = 128
SEQ = 128
PROMPTS = 4
TOKENS = PROMPTS * SEQ
SCORED = 256
NP = 32
NT = 8
FB = D // NT
ROWS = TOKENS // NP
QCOLS = 512
KVCOL = 128
WCOLS = QCOLS + 2 * KVCOL
EPSILON = 1e-05
THETA = 500000.0
MESH = pl.DeviceIdType.MESH
F32 = jnp.float32
BF16 = jnp.bfloat16
N_SENDS = 31


class PatchGather:
    def __init__(self, own, buf, send, recv):
        self.own, self.buf, self.send, self.recv = own, buf, send, recv
        me = lax.axis_index("patch")
        self.me = me
        self.x, self.z, self.c = me // 8, (me // 2) % 4, me % 2
        self.started = []

    def block(self, dx, dz, other=False):
        c = 1 - self.c if other else self.c
        return ((self.x + dx) % 4) * 8 + ((self.z + dz) % 4) * 2 + c

    def copy(self, src, index, target, slot):
        return pltpu.make_async_remote_copy(
            src_ref=src,
            dst_ref=self.buf.at[index],
            send_sem=self.send.at[slot],
            recv_sem=self.recv.at[index],
            device_id={"patch": target},
            device_id_type=MESH,
        )

    def start(self, src, index, target):
        c = self.copy(src, index, target, len(self.started))
        c.start()
        self.started.append(c)

    def wait(self, index):
        self.copy(self.buf.at[index], index, self.block(1, 0), 0).wait_recv()

    def z_send(self):
        for dz in (1, 3, 2):
            self.start(self.own, self.me, self.block(0, dz))

    def own_send(self):
        for target in (self.block(1, 0), self.block(3, 0), self.block(0, 0, True)):
            self.start(self.own, self.me, target)

    def z_forward(self, then=None):
        for dz in (3, 1, 2):
            b = self.block(0, dz)
            self.wait(b)
            for target in (self.block(1, 0), self.block(3, 0), self.block(0, 0, True)):
                self.start(self.buf.at[b], b, target)
            if then is not None:
                then(b)

    def x_forward(self, then=None):
        for dz in (0, 3, 1, 2):
            b = self.block(3, dz)
            self.wait(b)
            if dz in (0, 3):
                self.start(self.buf.at[b], b, self.block(1, 0))
            self.start(self.buf.at[b], b, self.block(0, 0, True))
            if then is not None:
                then(b)
            b = self.block(1, dz)
            self.wait(b)
            if dz in (1, 2):
                self.start(self.buf.at[b], b, self.block(3, 0))
            self.start(self.buf.at[b], b, self.block(0, 0, True))
            if then is not None:
                then(b)

    def far(self, then=None):
        for dz in (0, 3, 1, 2):
            b = self.block(2, dz)
            self.wait(b)
            self.start(self.buf.at[b], b, self.block(0, 0, True))
            if then is not None:
                then(b)

    def core_wait(self, then=None):
        for dx, dz in [(0, 0), (0, 3), (0, 1), (0, 2)] + [
            (dx, dz) for dz in (0, 3, 1, 2) for dx in (3, 1)
        ] + [(2, dz) for dz in (0, 3, 1, 2)]:
            b = self.block(dx, dz, True)
            self.wait(b)
            if then is not None:
                then(b)

    def drain(self):
        for c in self.started:
            c.wait_send()


def greet(targets):
    barrier = pltpu.get_barrier_semaphore()
    for target in targets:
        pl.semaphore_signal(barrier, inc=1, device_id=target, device_id_type=MESH)
    pl.semaphore_wait(barrier, len(targets))


def layer_kernel(
    xin, w_ref, wo_ref, clean_ref, corrupt_ref, early_ref, late_ref, cos_ref, sin_ref, gain_ref,
    fin_ref, ssq_ref,
    xrecv, nbuf, wbuf, acc, qown, qbuf, obuf, cbuf, att, part, got,
    x_send, x_recv, w_send, w_recv, q_send, q_recv, o_send, o_recv, c_send, c_recv, r_send, r_recv,
):
    t = lax.axis_index("tp")
    w = PatchGather(w_ref, wbuf, w_send, w_recv)
    q = PatchGather(qown, qbuf, q_send, q_recv)
    o = PatchGather(wo_ref, obuf, o_send, o_recv)
    cl = PatchGather(clean_ref, cbuf, c_send, c_recv)
    me = w.me
    others = [(t + k) % NT for k in range(1, NT)]
    greet(
        [{"tp": k} for k in others]
        + [{"patch": w.block(0, dz)} for dz in (1, 3, 2)]
        + [{"patch": b} for b in (w.block(1, 0), w.block(3, 0), w.block(0, 0, True))]
    )

    def x_copy(k, target):
        return pltpu.make_async_remote_copy(
            src_ref=xin, dst_ref=xrecv.at[t], send_sem=x_send.at[k], recv_sem=x_recv.at[t],
            device_id={"tp": target}, device_id_type=MESH,
        )

    x_copies = [x_copy(k, target) for k, target in enumerate(others)]
    for c in x_copies:
        c.start()
    w.z_send()
    w.own_send()
    o.z_send()
    cl.z_send()
    obuf[me] = wo_ref[...]
    cbuf[me] = clean_ref[...]
    xrecv[t] = xin[...]

    for target in others:
        pltpu.make_async_remote_copy(
            src_ref=xin, dst_ref=xrecv.at[target], send_sem=x_send.at[0], recv_sem=x_recv.at[target],
            device_id={"tp": target}, device_id_type=MESH,
        ).wait_recv()
    total = jnp.zeros((2 * ROWS, 1), F32)
    for k in range(NT):
        v = xrecv[k, : 2 * ROWS, :].astype(F32)
        total = total + jnp.sum(v * v, axis=1, keepdims=True)
    scale = lax.rsqrt(total / D + EPSILON)
    for k in range(NT):
        v = xrecv[k, : 2 * ROWS, :].astype(F32)
        g = xrecv[k, 2 * ROWS :, :].astype(F32)[:1]
        v = (v * scale * g).astype(BF16)
        for j in range(4):
            nbuf[4 * k + j] = v[:, 128 * j : 128 * (j + 1)]

    acc[...] = jnp.dot(nbuf[me], w_ref[...], preferred_element_type=F32)

    def add(b):
        acc[...] += jnp.dot(nbuf[b], wbuf[b], preferred_element_type=F32)

    w.z_forward(add)
    w.x_forward(add)
    o.own_send()
    o.z_forward()
    w.far(add)
    w.core_wait(add)

    cosine, sine = cos_ref[...], sin_ref[...]
    for h in range(WCOLS // HD):
        v = acc[:, HD * h : HD * (h + 1)]
        if h < 5:
            v = v * cosine + pltpu.roll(v, HD // 2, 1) * sine
        v = v.astype(BF16)
        for s in range(2):
            qown[s, :, HD * h : HD * (h + 1)] = v[ROWS * s : ROWS * (s + 1)]
    q.z_send()
    q.own_send()
    qbuf[me] = qown[...]
    q.z_forward()
    q.x_forward()
    q.far()
    cl.own_send()
    cl.z_forward()
    o.x_forward()
    o.far()
    q.core_wait()
    o.core_wait()

    early = early_ref[...] > 0.5
    row = lax.broadcasted_iota(jnp.int32, (4 * SEQ, SEQ), 0) % SEQ
    col = lax.broadcasted_iota(jnp.int32, (4 * SEQ, SEQ), 1)
    causal = row >= col

    def r_copy(k, n, target):
        rows = pl.ds(SEQ * n, SEQ)
        return pltpu.make_async_remote_copy(
            src_ref=part.at[target, rows], dst_ref=got.at[t, rows],
            send_sem=r_send.at[k, n], recv_sem=r_recv.at[t, n],
            device_id={"tp": target}, device_id_type=MESH,
        )

    r_copies = []
    for n in range(PROMPTS):
        def picked(lo, hi, n=n):
            a = qbuf[8 * n : 8 * (n + 1), 0, :, lo:hi].reshape(SEQ, hi - lo).astype(F32)
            b = qbuf[8 * n : 8 * (n + 1), 1, :, lo:hi].reshape(SEQ, hi - lo).astype(F32)
            return jnp.where(early, b, a).astype(BF16)

        queries = jnp.concatenate([picked(HD * h, HD * (h + 1)) for h in range(4)], axis=0)
        keys = picked(QCOLS, QCOLS + HD)
        values = picked(QCOLS + HD, QCOLS + 2 * HD)
        scores = lax.dot_general(
            queries, keys, (((1,), (1,)), ((), ())), preferred_element_type=F32
        ) * HD ** (-0.5)
        scores = jnp.where(causal, scores, -1e30)
        scores = jnp.exp(scores - jnp.max(scores, axis=1, keepdims=True))
        probs = (scores / jnp.sum(scores, axis=1, keepdims=True)).astype(BF16)
        heads = jnp.dot(probs, values, preferred_element_type=F32).astype(BF16)
        for h in range(4):
            att[:, HD * h : HD * (h + 1)] = heads[SEQ * h : SEQ * (h + 1)]
        rows = pl.ds(SEQ * n, SEQ)
        for k, target in enumerate(others + [t]):
            for j in range(2):
                b = 4 * target + 2 * j
                both = jnp.concatenate([obuf[b], obuf[b + 1]], axis=1)
                piece = jnp.dot(att[...], both, preferred_element_type=F32)
                part[target, rows, 256 * j : 256 * (j + 1)] = piece.astype(BF16)
            if k < NT - 1:
                c = r_copy(k, n, target)
                c.start()
                r_copies.append(c)

    cl.x_forward()
    cl.far()
    cl.core_wait()

    gain = gain_ref[...].astype(F32)
    for n in range(PROMPTS):
        rows = pl.ds(SEQ * n, SEQ)
        for target in others:
            pltpu.make_async_remote_copy(
                src_ref=part.at[target, rows], dst_ref=got.at[target, rows],
                send_sem=r_send.at[0, n], recv_sem=r_recv.at[target, n],
                device_id={"tp": target}, device_id_type=MESH,
            ).wait_recv()

        def finish(i, carry, n=n):
            at = pl.ds(pl.multiple_of(SEQ * n + ROWS * i, ROWS), ROWS)
            local = pl.ds(pl.multiple_of(ROWS * i, ROWS), ROWS)
            e = early_ref[local, :1] > 0.5
            late = late_ref[local, :1] > 0.5
            v = corrupt_ref[at, :].astype(F32)
            v = jnp.where(e, cbuf[8 * n + i, 0].astype(F32), v)
            head = part[t, at, :].astype(F32)
            for target in others:
                head = head + got[target, at, :].astype(F32)
            v = v + head
            v = jnp.where(late, cbuf[8 * n + i, 1].astype(F32), v)
            ssq_ref[at, :] = jnp.broadcast_to(jnp.sum(v * v, axis=1, keepdims=True), (ROWS, 128))
            fin_ref[at, :] = (v * gain).astype(BF16)
            return carry

        lax.fori_loop(0, SEQ // ROWS, finish, 0)

    for c in x_copies + r_copies:
        c.wait_send()
    for g in (w, q, o, cl):
        g.drain()


def layer(xin, wqkv, wout, clean, corrupt, early, late, cosine, sine, gain):
    vmem = pl.BlockSpec(memory_space=pltpu.VMEM)
    dma = pltpu.SemaphoreType.DMA
    return pl.pallas_call(
        layer_kernel,
        out_shape=(
            jax.ShapeDtypeStruct((TOKENS, FB), BF16),
            jax.ShapeDtypeStruct((TOKENS, 128), F32),
        ),
        in_specs=[vmem] * 10,
        out_specs=(vmem, vmem),
        scratch_shapes=[
            pltpu.VMEM((NT, 3 * ROWS, FB), BF16),
            pltpu.VMEM((NP, 2 * ROWS, 128), BF16),
            pltpu.VMEM((NP, 128, WCOLS), BF16),
            pltpu.VMEM((2 * ROWS, WCOLS), F32),
            pltpu.VMEM((2, ROWS, WCOLS), BF16),
            pltpu.VMEM((NP, 2, ROWS, WCOLS), BF16),
            pltpu.VMEM((NP, FB, 128), BF16),
            pltpu.VMEM((NP, 2, ROWS, FB), BF16),
            pltpu.VMEM((SEQ, FB), BF16),
            pltpu.VMEM((NT, TOKENS, FB), BF16),
            pltpu.VMEM((NT, TOKENS, FB), BF16),
            dma((NT,)), dma((NT,)),
            dma((N_SENDS,)), dma((NP,)),
            dma((N_SENDS,)), dma((NP,)),
            dma((N_SENDS,)), dma((NP,)),
            dma((N_SENDS,)), dma((NP,)),
            dma((NT, PROMPTS)), dma((NT, PROMPTS)),
        ],
        compiler_params=pltpu.CompilerParams(
            collective_id=0, has_side_effects=True, vmem_limit_bytes=56 * 1024 * 1024
        ),
        cost_estimate=pl.CostEstimate(
            flops=4 * 10**9, bytes_accessed=20 * 2**20, transcendentals=10**6
        ),
        name="layer",
    )(xin, wqkv, wout, clean, corrupt, early, late, cosine, sine, gain)


def logits_kernel(fin_ref, ssq_ref, score_ref, base_ref, out_ref, lg, lgot, sgot, l_send, l_recv, s_send, s_recv):
    t = lax.axis_index("tp")
    others = [(t + k) % NT for k in range(1, NT)]
    greet([{"tp": k} for k in others])
    part = TOKENS // NT

    def s_copy(k, target, to):
        return pltpu.make_async_remote_copy(
            src_ref=ssq_ref.at[pl.ds(pl.multiple_of(part * target, part), part)], dst_ref=sgot.at[to],
            send_sem=s_send.at[k], recv_sem=s_recv.at[to],
            device_id={"tp": target}, device_id_type=MESH,
        )

    def l_copy(k, target, to):
        return pltpu.make_async_remote_copy(
            src_ref=lg.at[target], dst_ref=lgot.at[to],
            send_sem=l_send.at[k], recv_sem=l_recv.at[to],
            device_id={"tp": target}, device_id_type=MESH,
        )

    copies = []
    for k, target in enumerate(others):
        copies.append(s_copy(k, target, t))
        copies[-1].start()
    value = lax.dot_general(
        fin_ref[...], score_ref[...], (((1,), (1,)), ((), ())), preferred_element_type=F32
    ).astype(BF16)
    lg[...] = value.reshape(NT, part, SCORED)
    for k, target in enumerate(others):
        copies.append(l_copy(k, target, t))
        copies[-1].start()
    logits = lg[t].astype(F32)
    total = ssq_ref[pl.ds(pl.multiple_of(part * t, part), part), :]
    for target in others:
        s_copy(0, target, target).wait_recv()
        l_copy(0, target, target).wait_recv()
        logits = logits + lgot[target].astype(F32)
        total = total + sgot[target]
    scale = lax.rsqrt(total / D + EPSILON)
    out_ref[...] = logits * scale[:, :1] - base_ref[...]
    for c in copies:
        c.wait_send()


def logits_call(fin, ssq, score, base):
    vmem = pl.BlockSpec(memory_space=pltpu.VMEM)
    dma = pltpu.SemaphoreType.DMA
    part = TOKENS // NT
    return pl.pallas_call(
        logits_kernel,
        out_shape=jax.ShapeDtypeStruct((part, SCORED), F32),
        in_specs=[vmem] * 4,
        out_specs=vmem,
        scratch_shapes=[
            pltpu.VMEM((NT, part, SCORED), BF16),
            pltpu.VMEM((NT, part, SCORED), BF16),
            pltpu.VMEM((NT, part, 128), F32),
            dma((NT,)), dma((NT,)), dma((NT,)), dma((NT,)),
        ],
        compiler_params=pltpu.CompilerParams(collective_id=1, has_side_effects=True),
        cost_estimate=pl.CostEstimate(
            flops=2 * 10**8, bytes_accessed=2**21, transcendentals=1000
        ),
        name="logits",
    )(fin, ssq, score, base)


def rope_rows(first):
    half = HD // 2
    freqs = THETA ** (-(jnp.arange(half, dtype=F32) * 2.0 / HD))
    angles = (first + jnp.arange(ROWS)).astype(F32)[:, None] * freqs[None, :]
    cosine, sine = jnp.cos(angles), jnp.sin(angles)
    return (
        jnp.tile(jnp.concatenate([cosine, cosine], axis=1), (2, 1)),
        jnp.tile(jnp.concatenate([-sine, sine], axis=1), (2, 1)),
    )


def on_device(
    resid_corrupt, resid_clean, patch_level, patch_mask, norm_gain, final_gain,
    w_query, w_key, w_value, w_out, unembed, scored_ids, base_logits,
):
    p = lax.axis_index("patch")
    t = lax.axis_index("tp")
    rows_dev = unembed.shape[0]
    first_row = (p * NT + t) * rows_dev
    owned_rows = (scored_ids[:, None] == first_row + lax.iota(jnp.int32, rows_dev)[None, :]).astype(BF16)
    chosen = jnp.dot(owned_rows, unembed, preferred_element_type=F32).astype(BF16)
    score_all = lax.psum(chosen, ("patch", "tp"))

    level = patch_level[0]
    spliced = patch_mask[0][:, None] == 1
    early = jnp.broadcast_to((spliced & (level == 0)).astype(F32), (SEQ, 128))
    late = jnp.broadcast_to((spliced & (level == 1)).astype(F32), (SEQ, 128))
    xin = jnp.concatenate(
        [
            lax.dynamic_slice_in_dim(resid_corrupt, p * ROWS, ROWS, axis=0),
            resid_clean[0],
            jnp.broadcast_to(norm_gain[None, :], (ROWS, FB)),
        ],
        axis=0,
    )
    wqkv = jnp.concatenate([w_query, w_key, w_value], axis=1)
    cosine, sine = rope_rows((p * ROWS) % SEQ)
    fin, ssq = layer(
        xin, wqkv, w_out, resid_clean, resid_corrupt, early, late, cosine, sine, final_gain[None, :]
    )
    score = lax.dynamic_slice_in_dim(score_all, t * FB, FB, axis=1)
    return logits_call(fin, ssq, score, base_logits)[None]


def solution(mesh):
    placed = (
        P(None, "tp"),
        P(None, "patch", "tp"),
        P("patch"),
        P("patch", None),
        P("tp"),
        P("tp"),
        P("patch", "tp"),
        P("patch", "tp"),
        P("patch", "tp"),
        P("tp", "patch"),
        P(("patch", "tp"), None),
        P(),
        P("tp", None),
    )
    return jax.shard_map(
        on_device, mesh=mesh, in_specs=placed, out_specs=P("patch", "tp", None), check_vma=False
    )
```

```python
import jax
import jax.numpy as jnp
import numpy as np
from jax import lax
from jax.experimental import pallas as pl
from jax.experimental.pallas import tpu as pltpu
from jax.sharding import PartitionSpec as P

D = 4096
HD = 128
SEQ = 128
PROMPTS = 4
TOKENS = PROMPTS * SEQ
SCORED = 256
NP = 32
NT = 8
FB = D // NT
ROWS = TOKENS // NP
QCOLS = 512
KVCOL = 128
WCOLS = QCOLS + 2 * KVCOL
EPSILON = 1e-05
THETA = 500000.0
MESH = pl.DeviceIdType.MESH
F32 = jnp.float32
BF16 = jnp.bfloat16
N_SENDS = 31


class PatchGather:
    def __init__(self, own, buf, send, recv):
        self.own, self.buf, self.send, self.recv = own, buf, send, recv
        me = lax.axis_index("patch")
        self.me = me
        self.x, self.z, self.c = me // 8, (me // 2) % 4, me % 2
        self.started = []

    def block(self, dx, dz, other=False):
        c = 1 - self.c if other else self.c
        return ((self.x + dx) % 4) * 8 + ((self.z + dz) % 4) * 2 + c

    def copy(self, src, index, target, slot):
        return pltpu.make_async_remote_copy(
            src_ref=src,
            dst_ref=self.buf.at[index],
            send_sem=self.send.at[slot],
            recv_sem=self.recv.at[index],
            device_id={"patch": target},
            device_id_type=MESH,
        )

    def start(self, src, index, target):
        c = self.copy(src, index, target, len(self.started))
        c.start()
        self.started.append(c)

    def wait(self, index):
        self.copy(self.buf.at[index], index, self.block(1, 0), 0).wait_recv()

    def z_send(self):
        for dz in (1, 3, 2):
            self.start(self.own, self.me, self.block(0, dz))

    def own_send(self):
        for target in (self.block(1, 0), self.block(3, 0), self.block(0, 0, True)):
            self.start(self.own, self.me, target)

    def z_forward(self, then=None):
        for dz in (3, 1, 2):
            b = self.block(0, dz)
            self.wait(b)
            for target in (self.block(1, 0), self.block(3, 0), self.block(0, 0, True)):
                self.start(self.buf.at[b], b, target)
            if then is not None:
                then(b)

    def x_forward(self, then=None):
        for dz in (0, 3, 1, 2):
            b = self.block(3, dz)
            self.wait(b)
            if dz in (0, 3):
                self.start(self.buf.at[b], b, self.block(1, 0))
            self.start(self.buf.at[b], b, self.block(0, 0, True))
            if then is not None:
                then(b)
            b = self.block(1, dz)
            self.wait(b)
            if dz in (1, 2):
                self.start(self.buf.at[b], b, self.block(3, 0))
            self.start(self.buf.at[b], b, self.block(0, 0, True))
            if then is not None:
                then(b)

    def far(self, then=None):
        for dz in (0, 3, 1, 2):
            b = self.block(2, dz)
            self.wait(b)
            self.start(self.buf.at[b], b, self.block(0, 0, True))
            if then is not None:
                then(b)

    def core_wait(self, then=None):
        for dx, dz in [(0, 0), (0, 3), (0, 1), (0, 2)] + [
            (dx, dz) for dz in (0, 3, 1, 2) for dx in (3, 1)
        ] + [(2, dz) for dz in (0, 3, 1, 2)]:
            b = self.block(dx, dz, True)
            self.wait(b)
            if then is not None:
                then(b)

    def drain(self):
        for c in self.started:
            c.wait_send()


def greet(targets):
    barrier = pltpu.get_barrier_semaphore()
    for target in targets:
        pl.semaphore_signal(barrier, inc=1, device_id=target, device_id_type=MESH)
    pl.semaphore_wait(barrier, len(targets))


def layer_kernel(
    corrupt_hbm, clean_hbm, wq_hbm, wk_hbm, wv_hbm, wo_hbm, unembed_hbm,
    level_ref, mask_ref, ids_ref, ngain_ref, fgain_ref, cos_ref, sin_ref, base_ref,
    out_ref,
    corrupt_ref, clean_ref, w_ref, wo_ref, unembed_ref,
    xin, xrecv, nbuf, wbuf, acc, qown, qbuf, obuf, cbuf, att, part, got, early_ref, late_ref,
    chosen, chosen_got, paired, spread, spread_z, sum_z, sum_x, own_x, score, fin, ssq, ssq_got, lg, lg_got,
    local, x_send, x_recv, w_send, w_recv, q_send, q_recv, o_send, o_recv, c_send, c_recv, r_send, r_recv,
    s_send, s_recv, sz_recv, sx_recv, sg_recv, l_send, l_recv, n_send, n_recv,
):
    t = lax.axis_index("tp")
    w = PatchGather(w_ref, wbuf, w_send, w_recv)
    q = PatchGather(qown, qbuf, q_send, q_recv)
    o = PatchGather(wo_ref, obuf, o_send, o_recv)
    cl = PatchGather(clean_ref, cbuf, c_send, c_recv)
    me, px, pz, pc = w.me, w.x, w.z, w.c
    others = [(t + k) % NT for k in range(1, NT)]
    z_others = [(k, (pz + k) % 4) for k in (1, 3, 2)]
    x_others = [(k, (px + k) % 4) for k in (1, 3, 2)]
    partner = w.block(0, 0, True)

    loads = [
        pltpu.make_async_copy(src, dst, local.at[k])
        for k, (src, dst) in enumerate(
            [
                (wq_hbm, w_ref.at[:, pl.ds(0, QCOLS)]),
                (wk_hbm, w_ref.at[:, pl.ds(QCOLS, KVCOL)]),
                (wv_hbm, w_ref.at[:, pl.ds(QCOLS + KVCOL, KVCOL)]),
                (clean_hbm, clean_ref),
                (wo_hbm, wo_ref),
                (corrupt_hbm, corrupt_ref),
                (unembed_hbm, unembed_ref),
            ]
        )
    ]
    for c in loads:
        c.start()
    for c in loads[:6]:
        c.wait()
    xin[:ROWS] = corrupt_ref[pl.ds(pl.multiple_of(me * ROWS, ROWS), ROWS), :]
    xin[ROWS : 2 * ROWS] = clean_ref[0]
    xin[2 * ROWS :] = jnp.broadcast_to(ngain_ref[...].astype(F32), (ROWS, FB)).astype(BF16)
    spliced = jnp.transpose(jnp.broadcast_to(mask_ref[...].astype(F32), (SEQ, SEQ)))
    level = level_ref[0].astype(F32)
    early_ref[...] = spliced * (1.0 - level)
    late_ref[...] = spliced * level
    obuf[me] = wo_ref[...]
    cbuf[me] = clean_ref[...]
    xrecv[t] = xin[...]
    greet(
        [{"tp": k} for k in others]
        + [{"patch": w.block(0, dz)} for dz in (1, 3, 2)]
        + [{"patch": w.block(dx, 0)} for dx in (1, 3, 2)]
        + [{"patch": partner}]
    )

    def x_copy(k, target):
        return pltpu.make_async_remote_copy(
            src_ref=xin, dst_ref=xrecv.at[t], send_sem=x_send.at[k], recv_sem=x_recv.at[t],
            device_id={"tp": target}, device_id_type=MESH,
        )

    started = [x_copy(k, target) for k, target in enumerate(others)]
    for c in started:
        c.start()
    w.z_send()
    w.own_send()
    o.z_send()
    cl.z_send()

    def s_copy(src, dst, send, recv, where):
        return pltpu.make_async_remote_copy(
            src_ref=src, dst_ref=dst, send_sem=s_send.at[send], recv_sem=recv,
            device_id=where, device_id_type=MESH,
        )

    def begin(c):
        c.start()
        started.append(c)

    loads[6].wait()
    rows_dev = unembed_ref.shape[0]
    wanted = ids_ref[...] - (me * NT + t) * rows_dev
    owned = jnp.where(
        wanted == lax.broadcasted_iota(jnp.int32, (SCORED, rows_dev), 1), 1.0, 0.0
    ).astype(BF16)
    for k in range(NT):
        chosen[k] = jnp.dot(
            owned, unembed_ref[:, FB * k : FB * (k + 1)], preferred_element_type=F32
        ).astype(BF16)
    half = SCORED // 2
    pair = s_copy(
        chosen.at[:, pl.ds(pl.multiple_of(half * (1 - pc), half), half)],
        chosen_got, 0, s_recv.at[0], {"patch": partner},
    )
    begin(pair)

    for target in others:
        pltpu.make_async_remote_copy(
            src_ref=xin, dst_ref=xrecv.at[target], send_sem=x_send.at[0], recv_sem=x_recv.at[target],
            device_id={"tp": target}, device_id_type=MESH,
        ).wait_recv()
    total = jnp.zeros((2 * ROWS, 1), F32)
    for k in range(NT):
        v = xrecv[k, : 2 * ROWS, :].astype(F32)
        total = total + jnp.sum(v * v, axis=1, keepdims=True)
    scale = lax.rsqrt(total / D + EPSILON)
    for k in range(NT):
        v = xrecv[k, : 2 * ROWS, :].astype(F32)
        g = xrecv[k, 2 * ROWS :, :].astype(F32)[:1]
        v = (v * scale * g).astype(BF16)
        for j in range(4):
            nbuf[4 * k + j] = v[:, 128 * j : 128 * (j + 1)]

    acc[...] = jnp.dot(nbuf[me], w_ref[...], preferred_element_type=F32)

    def add(b):
        acc[...] += jnp.dot(nbuf[b], wbuf[b], preferred_element_type=F32)

    w.z_forward(add)

    pair.wait_recv()
    paired[...] = chosen[:, pl.ds(pl.multiple_of(half * pc, half), half)] + chosen_got[...]
    for k, target in enumerate(others):
        begin(s_copy(paired.at[target], spread.at[t], 1 + k, s_recv.at[1 + t], {"tp": target}))

    w.x_forward(add)
    o.own_send()
    o.z_forward()

    v = paired[t]
    for target in others:
        s_copy(paired.at[target], spread.at[target], 0, s_recv.at[1 + target], {"tp": target}).wait_recv()
        v = v + spread[target]
    spread_z[...] = v.reshape(4, half // 4, FB)
    for k, target in z_others:
        begin(s_copy(spread_z.at[target], sum_z.at[pz], 8 + k, sz_recv.at[pz], {"patch": w.block(0, k)}))

    w.far(add)
    w.core_wait(add)

    at = pl.ds(pl.multiple_of((me * ROWS) % SEQ, ROWS), ROWS)
    cosine = jnp.concatenate([cos_ref[at, :]] * 2, axis=0)
    sine = jnp.concatenate([sin_ref[at, :]] * 2, axis=0)
    for h in range(WCOLS // HD):
        v = acc[:, HD * h : HD * (h + 1)]
        if h < 5:
            v = v * cosine + pltpu.roll(v, HD // 2, 1) * sine
        v = v.astype(BF16)
        for s in range(2):
            qown[s, :, HD * h : HD * (h + 1)] = v[ROWS * s : ROWS * (s + 1)]
    q.z_send()
    q.own_send()
    qbuf[me] = qown[...]

    v = spread_z[pz]
    for k, target in z_others:
        s_copy(spread_z.at[target], sum_z.at[target], 0, sz_recv.at[target], {"patch": w.block(0, k)}).wait_recv()
        v = v + sum_z[target]
    own_x[...] = v
    for k, target in x_others:
        begin(s_copy(own_x, sum_x.at[px], 12 + k, sx_recv.at[px], {"patch": w.block(k, 0)}))

    q.z_forward()
    q.x_forward()

    v = own_x[...]
    for k, target in x_others:
        s_copy(own_x, sum_x.at[target], 0, sx_recv.at[target], {"patch": w.block(k, 0)}).wait_recv()
        v = v + sum_x[target]
    score[pc, pz] = v
    for k, target in z_others:
        begin(s_copy(score.at[pc, pz], score.at[pc, pz], 16 + k, sg_recv.at[pz], {"patch": w.block(0, k)}))

    q.far()
    cl.own_send()
    cl.z_forward()
    o.x_forward()
    o.far()
    for k, target in z_others:
        s_copy(score.at[pc, target], score.at[pc, target], 0, sg_recv.at[target], {"patch": w.block(0, k)}).wait_recv()
    begin(s_copy(score.at[pc], score.at[pc], 20, s_recv.at[9], {"patch": partner}))
    q.core_wait()
    o.core_wait()

    early = early_ref[...] > 0.5
    row = lax.broadcasted_iota(jnp.int32, (4 * SEQ, SEQ), 0) % SEQ
    col = lax.broadcasted_iota(jnp.int32, (4 * SEQ, SEQ), 1)
    causal = row >= col

    def r_copy(k, n, target, to):
        rows = pl.ds(SEQ * n, SEQ)
        return pltpu.make_async_remote_copy(
            src_ref=part.at[target, rows], dst_ref=got.at[to, rows],
            send_sem=r_send.at[k, n], recv_sem=r_recv.at[to, n],
            device_id={"tp": target}, device_id_type=MESH,
        )

    for n in range(PROMPTS):
        def picked(lo, hi, n=n):
            a = qbuf[8 * n : 8 * (n + 1), 0, :, lo:hi].reshape(SEQ, hi - lo).astype(F32)
            b = qbuf[8 * n : 8 * (n + 1), 1, :, lo:hi].reshape(SEQ, hi - lo).astype(F32)
            return jnp.where(early, b, a).astype(BF16)

        queries = jnp.concatenate([picked(HD * h, HD * (h + 1)) for h in range(4)], axis=0)
        keys = picked(QCOLS, QCOLS + HD)
        values = picked(QCOLS + HD, QCOLS + 2 * HD)
        scores = lax.dot_general(
            queries, keys, (((1,), (1,)), ((), ())), preferred_element_type=F32
        ) * HD ** (-0.5)
        scores = jnp.where(causal, scores, -1e30)
        scores = jnp.exp(scores - jnp.max(scores, axis=1, keepdims=True))
        probs = (scores / jnp.sum(scores, axis=1, keepdims=True)).astype(BF16)
        heads = jnp.dot(probs, values, preferred_element_type=F32).astype(BF16)
        for h in range(4):
            att[:, HD * h : HD * (h + 1)] = heads[SEQ * h : SEQ * (h + 1)]
        rows = pl.ds(SEQ * n, SEQ)
        for k, target in enumerate(others + [t]):
            for j in range(2):
                b = 4 * target + 2 * j
                both = jnp.concatenate([obuf[b], obuf[b + 1]], axis=1)
                piece = jnp.dot(att[...], both, preferred_element_type=F32)
                part[target, rows, 256 * j : 256 * (j + 1)] = piece.astype(BF16)
            if k < NT - 1:
                begin(r_copy(k, n, target, t))

    cl.x_forward()
    cl.far()
    cl.core_wait()
    s_copy(score.at[pc], score.at[1 - pc], 0, s_recv.at[9], {"patch": partner}).wait_recv()

    gain = fgain_ref[...].astype(F32)
    share = TOKENS // NT

    def l_copy(target, to):
        return pltpu.make_async_remote_copy(
            src_ref=lg.at[target], dst_ref=lg_got.at[to], send_sem=l_send.at[target], recv_sem=l_recv.at[to],
            device_id={"tp": target}, device_id_type=MESH,
        )

    def n_copy(target, to):
        return pltpu.make_async_remote_copy(
            src_ref=ssq.at[target], dst_ref=ssq_got.at[to], send_sem=n_send.at[target], recv_sem=n_recv.at[to],
            device_id={"tp": target}, device_id_type=MESH,
        )

    for n in range(PROMPTS):
        for target in others:
            r_copy(0, n, target, target).wait_recv()

        def finish(i, carry, n=n):
            at = pl.ds(pl.multiple_of(SEQ * n + ROWS * i, ROWS), ROWS)
            local_at = pl.ds(pl.multiple_of(ROWS * i, ROWS), ROWS)
            e = early_ref[local_at, :1] > 0.5
            late = late_ref[local_at, :1] > 0.5
            v = corrupt_ref[at, :].astype(F32)
            v = jnp.where(e, cbuf[8 * n + i, 0].astype(F32), v)
            head = part[t, at, :].astype(F32)
            for target in others:
                head = head + got[target, at, :].astype(F32)
            v = v + head
            v = jnp.where(late, cbuf[8 * n + i, 1].astype(F32), v)
            within = pl.ds(pl.multiple_of(ROWS * (i % 4), ROWS), ROWS)
            ssq[2 * n + i // 4, within, :] = jnp.broadcast_to(
                jnp.sum(v * v, axis=1, keepdims=True), (ROWS, 128)
            )
            fin[local_at, :] = (v * gain).astype(BF16)
            return carry

        lax.fori_loop(0, SEQ // ROWS, finish, 0)
        value = lax.dot_general(
            fin[...], score[...].reshape(SCORED, FB), (((1,), (1,)), ((), ())),
            preferred_element_type=F32,
        ).astype(BF16)
        for s in range(2):
            target = 2 * n + s
            lg[target] = value[share * s : share * (s + 1)]

            @pl.when(target != t)
            def _(target=target):
                n_copy(target, t).start()
                l_copy(target, t).start()

    logits = lg[t].astype(F32)
    total = ssq[t]
    for target in others:
        n_copy(target, target).wait_recv()
        l_copy(target, target).wait_recv()
        logits = logits + lg_got[target].astype(F32)
        total = total + ssq_got[target]
    scale = lax.rsqrt(total / D + EPSILON)
    out_ref[...] = logits * scale[:, :1] - base_ref[...]

    for target in others:
        n_copy(target, t).wait_send()
        l_copy(target, t).wait_send()
    for c in started:
        c.wait_send()
    for g in (w, q, o, cl):
        g.drain()


def layer(*operands):
    vmem = pl.BlockSpec(memory_space=pltpu.VMEM)
    smem = pl.BlockSpec(memory_space=pltpu.SMEM)
    hbm = pl.BlockSpec(memory_space=pl.ANY)
    dma = pltpu.SemaphoreType.DMA
    share = TOKENS // NT
    half = SCORED // 2
    rows_dev = operands[6].shape[0]
    return pl.pallas_call(
        layer_kernel,
        out_shape=jax.ShapeDtypeStruct((share, SCORED), F32),
        in_specs=[hbm] * 7 + [smem] + [vmem] * 7,
        out_specs=vmem,
        scratch_shapes=[
            pltpu.VMEM((TOKENS, FB), BF16),
            pltpu.VMEM((2, ROWS, FB), BF16),
            pltpu.VMEM((128, WCOLS), BF16),
            pltpu.VMEM((FB, 128), BF16),
            pltpu.VMEM((rows_dev, D), BF16),
            pltpu.VMEM((3 * ROWS, FB), BF16),
            pltpu.VMEM((NT, 3 * ROWS, FB), BF16),
            pltpu.VMEM((NP, 2 * ROWS, 128), BF16),
            pltpu.VMEM((NP, 128, WCOLS), BF16),
            pltpu.VMEM((2 * ROWS, WCOLS), F32),
            pltpu.VMEM((2, ROWS, WCOLS), BF16),
            pltpu.VMEM((NP, 2, ROWS, WCOLS), BF16),
            pltpu.VMEM((NP, FB, 128), BF16),
            pltpu.VMEM((NP, 2, ROWS, FB), BF16),
            pltpu.VMEM((SEQ, FB), BF16),
            pltpu.VMEM((NT, TOKENS, FB), BF16),
            pltpu.VMEM((NT, TOKENS, FB), BF16),
            pltpu.VMEM((SEQ, SEQ), F32),
            pltpu.VMEM((SEQ, SEQ), F32),
            pltpu.VMEM((NT, SCORED, FB), BF16),
            pltpu.VMEM((NT, half, FB), BF16),
            pltpu.VMEM((NT, half, FB), BF16),
            pltpu.VMEM((NT, half, FB), BF16),
            pltpu.VMEM((4, half // 4, FB), BF16),
            pltpu.VMEM((4, half // 4, FB), BF16),
            pltpu.VMEM((4, half // 4, FB), BF16),
            pltpu.VMEM((half // 4, FB), BF16),
            pltpu.VMEM((2, 4, half // 4, FB), BF16),
            pltpu.VMEM((SEQ, FB), BF16),
            pltpu.VMEM((NT, share, 128), F32),
            pltpu.VMEM((NT, share, 128), F32),
            pltpu.VMEM((NT, share, SCORED), BF16),
            pltpu.VMEM((NT, share, SCORED), BF16),
            dma((7,)),
            dma((NT,)), dma((NT,)),
            dma((N_SENDS,)), dma((NP,)),
            dma((N_SENDS,)), dma((NP,)),
            dma((N_SENDS,)), dma((NP,)),
            dma((N_SENDS,)), dma((NP,)),
            dma((NT, PROMPTS)), dma((NT, PROMPTS)),
            dma((21,)), dma((10,)), dma((4,)), dma((4,)), dma((4,)),
            dma((NT,)), dma((NT,)), dma((NT,)), dma((NT,)),
        ],
        compiler_params=pltpu.CompilerParams(
            collective_id=0, has_side_effects=True, vmem_limit_bytes=60 * 1024 * 1024
        ),
        cost_estimate=pl.CostEstimate(
            flops=4 * 10**9, bytes_accessed=20 * 2**20, transcendentals=10**6
        ),
        name="layer",
    )(*operands)


def rope_tables():
    half = HD // 2
    exponents = -(np.arange(half, dtype=np.float32) * np.float32(2.0 / HD))
    freqs = (np.float32(THETA) ** exponents).astype(np.float32)
    angles = np.arange(SEQ, dtype=np.float32)[:, None] * freqs[None, :]
    cosine, sine = np.cos(angles), np.sin(angles)
    return (
        np.concatenate([cosine, cosine], axis=1).astype(np.float32),
        np.concatenate([-sine, sine], axis=1).astype(np.float32),
    )


def on_device(
    resid_corrupt, resid_clean, patch_level, patch_mask, norm_gain, final_gain,
    w_query, w_key, w_value, w_out, unembed, scored_ids, base_logits,
):
    cosine, sine = rope_tables()
    out = layer(
        resid_corrupt, resid_clean, w_query, w_key, w_value, w_out, unembed,
        patch_level, patch_mask, scored_ids[:, None], norm_gain[None, :], final_gain[None, :],
        jnp.asarray(cosine), jnp.asarray(sine), base_logits,
    )
    return out[None]


def solution(mesh):
    placed = (
        P(None, "tp"),
        P(None, "patch", "tp"),
        P("patch"),
        P("patch", None),
        P("tp"),
        P("tp"),
        P("patch", "tp"),
        P("patch", "tp"),
        P("patch", "tp"),
        P("tp", "patch"),
        P(("patch", "tp"), None),
        P(),
        P("tp", None),
    )
    return jax.shard_map(
        on_device, mesh=mesh, in_specs=placed, out_specs=P("patch", "tp", None), check_vma=False
    )
```

```python
import jax
import jax.numpy as jnp
import numpy as np
from jax import lax
from jax.experimental import pallas as pl
from jax.experimental.pallas import tpu as pltpu
from jax.sharding import PartitionSpec as P

D = 4096
HD = 128
SEQ = 128
PROMPTS = 4
TOKENS = PROMPTS * SEQ
SCORED = 256
NP = 32
NT = 8
FB = D // NT
ROWS = TOKENS // NP
QCOLS = 512
KVCOL = 128
WCOLS = QCOLS + 2 * KVCOL
EPSILON = 1e-05
THETA = 500000.0
MESH = pl.DeviceIdType.MESH
F32 = jnp.float32
BF16 = jnp.bfloat16
N_SENDS = 31


class PatchGather:
    def __init__(self, own, buf, send, recv):
        self.own, self.buf, self.send, self.recv = own, buf, send, recv
        me = lax.axis_index("patch")
        self.me = me
        self.x, self.z, self.c = me // 8, (me // 2) % 4, me % 2
        self.way = 1 - 2 * self.c
        self.started = []

    def block(self, dx, dz, other=False):
        c = 1 - self.c if other else self.c
        return ((self.x + dx) % 4) * 8 + ((self.z + dz + 4) % 4) * 2 + c

    def copy(self, src, index, target, slot):
        return pltpu.make_async_remote_copy(
            src_ref=src,
            dst_ref=self.buf.at[index],
            send_sem=self.send.at[slot],
            recv_sem=self.recv.at[index],
            device_id={"patch": target},
            device_id_type=MESH,
        )

    def start(self, src, index, target):
        c = self.copy(src, index, target, len(self.started))
        c.start()
        self.started.append(c)

    def wait(self, index):
        self.copy(self.buf.at[index], index, self.block(1, 0), 0).wait_recv()

    def z_send(self):
        for dz in (self.way, -self.way):
            self.start(self.own, self.me, self.block(0, dz))

    def own_send(self):
        for target in (self.block(1, 0), self.block(3, 0), self.block(0, 0, True)):
            self.start(self.own, self.me, target)

    def z_relay(self):
        b = self.block(0, -self.way)
        self.wait(b)
        self.start(self.buf.at[b], b, self.block(0, self.way))

    def spread(self, b):
        for target in (self.block(1, 0), self.block(3, 0), self.block(0, 0, True)):
            self.start(self.buf.at[b], b, target)

    def z_forward(self, relayed=False):
        for k, dz in enumerate((-self.way, self.way, 2)):
            b = self.block(0, dz)
            if k > 0:
                self.wait(b)
            elif not relayed:
                self.z_relay()
            self.spread(b)
            if k == 0 and not relayed:
                self.x_near(0)

    def x_near(self, k, then=None):
        for dx in (3, 1):
            b = self.block(dx, (0, -self.way, self.way, 2)[k])
            self.wait(b)
            if (k < 2) == (dx == 3):
                self.start(self.buf.at[b], b, self.block(4 - dx, 0))
            self.start(self.buf.at[b], b, self.block(0, 0, True))
            if then is not None:
                then(b)

    def x_forward(self, then=None, first=1):
        for k in range(first, 4):
            self.x_near(k, then)

    def far(self, then=None):
        for dz in (0, -self.way, self.way, 2):
            b = self.block(2, dz)
            self.wait(b)
            self.start(self.buf.at[b], b, self.block(0, 0, True))
            if then is not None:
                then(b)

    def core_wait(self, then=None):
        z = (0, self.way, -self.way, 2)
        for dx, dz in [(0, dz) for dz in z] + [(dx, dz) for dz in z for dx in (3, 1)] + [(2, dz) for dz in z]:
            b = self.block(dx, dz, True)
            self.wait(b)
            if then is not None:
                then(b)

    def drain(self):
        for c in self.started:
            c.wait_send()


def layer_kernel(
    corrupt_hbm, clean_hbm, wq_hbm, wk_hbm, wv_hbm, wo_hbm, unembed_hbm,
    level_ref, mask_ref, ids_ref, gains_ref, cos_ref, sin_ref,
    out_ref,
    corrupt_ref, clean_ref, w_ref, wo_ref, wo_own, unembed_ref,
    xin, xrecv, nbuf, wbuf, acc, qown, qbuf, obuf, cbuf, att, head, early_ref, late_ref,
    chosen, chosen_got, paired, spread, mine, mine_got, spread_z, sum_z, sum_x, own_x, score, fin, score_t, squares, ssq, ssq_got, lg, lg_got,
    local, x_send, x_recv, w_send, w_recv, q_send, q_recv, o_send, o_recv, c_send, c_recv, a_send, a_recv,
    s_send, s_recv, sz_recv, sx_recv, sg_recv, l_send, l_recv, n_send, n_recv,
):
    t = lax.axis_index("tp")
    w = PatchGather(w_ref, wbuf, w_send, w_recv)
    q = PatchGather(qown, qbuf, q_send, q_recv)
    o = PatchGather(wo_own, obuf, o_send, o_recv)
    cl = PatchGather(clean_ref, cbuf, c_send, c_recv)
    me, px, pz, pc = w.me, w.x, w.z, w.c
    ty, tz = t // 2, t % 2
    beside = t + 1 - 2 * tz
    others = [(t + k) % NT for k in range(1, NT)]
    z_others = [(k, (pz + k) % 4) for k in (1, 3, 2)]
    x_others = [(k, (px + k) % 4) for k in (1, 3, 2)]
    partner = w.block(0, 0, True)
    swap_p, swap_t = 4 * t + me % 4, me // 4
    swaps = swap_t != t

    loads = [
        pltpu.make_async_copy(src, dst, local.at[k])
        for k, (src, dst) in enumerate(
            [
                (corrupt_hbm, corrupt_ref),
                (clean_hbm, clean_ref),
                (wq_hbm, w_ref.at[:, pl.ds(0, QCOLS)]),
                (wk_hbm, w_ref.at[:, pl.ds(QCOLS, KVCOL)]),
                (wv_hbm, w_ref.at[:, pl.ds(QCOLS + KVCOL, KVCOL)]),
                (wo_hbm, wo_ref),
                (unembed_hbm, unembed_ref),
            ]
        )
    ]
    for c in loads:
        c.start()
    barrier = pltpu.get_barrier_semaphore()
    peers = (
        [{"tp": k} for k in others]
        + [{"patch": w.block(0, dz)} for dz in (1, 3, 2)]
        + [{"patch": w.block(dx, 0)} for dx in (1, 3, 2)]
        + [{"patch": partner}]
    )
    for peer in peers:
        pl.semaphore_signal(barrier, inc=1, device_id=peer, device_id_type=MESH)

    @pl.when(swaps)
    def _():
        pl.semaphore_signal(
            barrier, inc=1, device_id={"patch": swap_p, "tp": swap_t}, device_id_type=MESH
        )

    for c in loads[:2]:
        c.wait()
    xin[:ROWS] = corrupt_ref[pl.ds(pl.multiple_of(me * ROWS, ROWS), ROWS), :]
    xin[ROWS : 2 * ROWS] = clean_ref[0]
    xin[2 * ROWS :] = jnp.broadcast_to(gains_ref[:1], (ROWS, FB)).astype(BF16)
    xrecv[t] = xin[...]
    spliced = jnp.transpose(jnp.broadcast_to(mask_ref[...].astype(F32), (SEQ, SEQ)))
    level = level_ref[0].astype(F32)
    early_ref[...] = spliced * (1.0 - level)
    late_ref[...] = spliced * level
    cbuf[me] = clean_ref[...]
    for c in loads[2:6]:
        c.wait()
    pl.semaphore_wait(barrier, len(peers) + swaps.astype(jnp.int32))

    started = []

    def begin(c):
        c.start()
        started.append(c)

    def x_copy(k, target, to):
        return pltpu.make_async_remote_copy(
            src_ref=xin, dst_ref=xrecv.at[to], send_sem=x_send.at[k], recv_sem=x_recv.at[to],
            device_id={"tp": target}, device_id_type=MESH,
        )

    def s_copy(src, dst, send, recv, where):
        return pltpu.make_async_remote_copy(
            src_ref=src, dst_ref=dst, send_sem=s_send.at[send], recv_sem=recv,
            device_id=where, device_id_type=MESH,
        )

    w.z_send()
    w.own_send()
    for k, target in enumerate(others):
        begin(x_copy(k, target, t))
    swap = s_copy(wo_ref, wo_own, 21, s_recv.at[10], {"patch": swap_p, "tp": swap_t})

    @pl.when(swaps)
    def _():
        swap.start()

    loads[6].wait()
    rows_dev = unembed_ref.shape[0]
    wanted = jnp.transpose(jnp.broadcast_to(ids_ref[...].astype(F32), (SCORED, SCORED)))[:, :1]
    wanted = wanted.astype(jnp.int32) - (me * NT + t) * rows_dev
    owned = jnp.where(
        wanted == lax.broadcasted_iota(jnp.int32, (SCORED, rows_dev), 1), 1.0, 0.0
    ).astype(BF16)
    for k in range(NT):
        chosen[k] = jnp.dot(
            owned, unembed_ref[:, FB * k : FB * (k + 1)], preferred_element_type=F32
        ).astype(BF16)
    half = SCORED // 2
    pair = s_copy(
        chosen.at[:, pl.ds(pl.multiple_of(half * (1 - pc), half), half)],
        chosen_got, 0, s_recv.at[0], {"patch": partner},
    )
    begin(pair)
    pair.wait_recv()
    paired[...] = (
        chosen[:, pl.ds(pl.multiple_of(half * pc, half), half)] + chosen_got[...]
    ).reshape(4, 2, half, FB)
    y_others = [(k, (ty + k) % 4) for k in (1, 3, 2)]
    for k, y in y_others:
        begin(s_copy(paired.at[y], spread.at[ty], k, s_recv.at[1 + ty], {"tp": 2 * y + tz}))

    w.z_forward()

    @pl.when(swaps)
    def _():
        swap.wait_recv()

    @pl.when(jnp.logical_not(swaps))
    def _():
        wo_own[...] = wo_ref[...]

    o.z_send()
    for target in others:
        x_copy(0, target, target).wait_recv()
    total = jnp.zeros((2 * ROWS, 1), F32)
    for k in range(NT):
        v = xrecv[k, : 2 * ROWS, :].astype(F32)
        total = total + jnp.sum(v * v, axis=1, keepdims=True)
    scale = lax.rsqrt(total / D + EPSILON)
    for k in range(NT):
        v = xrecv[k, : 2 * ROWS, :].astype(F32)
        g = xrecv[k, 2 * ROWS :, :].astype(F32)[:1]
        v = (v * scale * g).astype(BF16)
        for j in range(4):
            nbuf[4 * k + j] = v[:, 128 * j : 128 * (j + 1)]

    acc[...] = jnp.dot(nbuf[me], w_ref[...], preferred_element_type=F32)

    def add(b):
        acc[...] += jnp.dot(nbuf[b], wbuf[b], preferred_element_type=F32)

    for b in [w.block(0, dz) for dz in (3, 1, 2)] + [w.block(dx, 0) for dx in (3, 1)]:
        add(b)
    w.x_forward(add)
    obuf[me] = wo_own[...]
    o.z_relay()
    cl.z_send()

    v = paired[ty]
    for k, y in y_others:
        s_copy(paired.at[y], spread.at[y], 0, s_recv.at[1 + y], {"tp": 2 * y + tz}).wait_recv()
        v = v + spread[y]
    mine[...] = v
    begin(s_copy(mine.at[1 - tz], mine_got, 4, s_recv.at[5], {"tp": beside}))
    w.far(add)
    w.core_wait(add)

    at = pl.ds(pl.multiple_of((me * ROWS) % SEQ, ROWS), ROWS)
    cosine = jnp.concatenate([cos_ref[at, :]] * 2, axis=0)
    sine = jnp.concatenate([sin_ref[at, :]] * 2, axis=0)
    for h in range(WCOLS // HD):
        v = acc[:, HD * h : HD * (h + 1)]
        if h < 5:
            v = v * cosine + pltpu.roll(v, HD // 2, 1) * sine
        v = v.astype(BF16)
        for s in range(2):
            qown[s, :, HD * h : HD * (h + 1)] = v[ROWS * s : ROWS * (s + 1)]
    qbuf[me] = qown[...]
    q.z_send()
    q.own_send()
    cl.z_relay()
    q.z_forward()

    s_copy(mine.at[1 - tz], mine_got, 4, s_recv.at[5], {"tp": beside}).wait_recv()
    spread_z[...] = (mine[tz] + mine_got[...]).reshape(4, half // 4, FB)
    for k, target in z_others:
        begin(s_copy(spread_z.at[target], sum_z.at[pz], 8 + k, sz_recv.at[pz], {"patch": w.block(0, k)}))

    q.x_forward()
    o.own_send()
    o.z_forward(True)
    cl.own_send()
    cl.z_forward(True)
    q.far()

    v = spread_z[pz]
    for k, target in z_others:
        s_copy(spread_z.at[target], sum_z.at[target], 0, sz_recv.at[target], {"patch": w.block(0, k)}).wait_recv()
        v = v + sum_z[target]
    own_x[...] = v
    for k, target in x_others:
        begin(s_copy(own_x, sum_x.at[px], 12 + k, sx_recv.at[px], {"patch": w.block(k, 0)}))

    q.core_wait()

    early = early_ref[...] > 0.5
    row = lax.broadcasted_iota(jnp.int32, (4 * SEQ, SEQ), 0) % SEQ
    col = lax.broadcasted_iota(jnp.int32, (4 * SEQ, SEQ), 1)
    causal = row >= col

    def a_copy(index, n, source, target):
        rows = pl.ds(SEQ * n, SEQ)
        return pltpu.make_async_remote_copy(
            src_ref=att.at[source, rows], dst_ref=att.at[source, rows],
            send_sem=a_send.at[index], recv_sem=a_recv.at[source, n],
            device_id={"tp": target}, device_id_type=MESH,
        )

    a_count = []

    def a_start(n, source, target):
        begin(a_copy(len(a_count), n, source, target))
        a_count.append(n)

    def a_wait(n, source):
        a_copy(0, n, source, others[0]).wait_recv()

    up, down, far_y = ((ty + 1) % 4) * 2, ((ty + 3) % 4) * 2, ((ty + 2) % 4) * 2
    near = (down, up)

    def across(n):
        return n >= 2

    def clockwise(n):
        return n % 2 == 0

    def first(n):
        for y in near:
            a_wait(n, y + tz)
            if clockwise(n) == (y is down):
                a_start(n, y + tz, (up if y is down else down) + tz)
            if across(n):
                a_start(n, y + tz, beside)
        a_wait(n, beside)
        if not across(n):
            a_start(n, beside, up + tz)
            a_start(n, beside, down + tz)

    def second(n):
        a_wait(n, far_y + tz)
        if across(n):
            a_start(n, far_y + tz, beside)
        for y in near:
            a_wait(n, y + 1 - tz)
            if not across(n) and clockwise(n) == (y is down):
                a_start(n, y + 1 - tz, (up if y is down else down) + tz)

    def third(n):
        a_wait(n, far_y + 1 - tz)

    for n in range(PROMPTS):
        def picked(lo, hi, n=n):
            a = qbuf[8 * n : 8 * (n + 1), 0, :, lo:hi].reshape(SEQ, hi - lo).astype(F32)
            b = qbuf[8 * n : 8 * (n + 1), 1, :, lo:hi].reshape(SEQ, hi - lo).astype(F32)
            return jnp.where(early, b, a).astype(BF16)

        queries = jnp.concatenate([picked(HD * h, HD * (h + 1)) for h in range(4)], axis=0)
        keys = picked(QCOLS, QCOLS + HD)
        values = picked(QCOLS + HD, QCOLS + 2 * HD)
        scores = lax.dot_general(
            queries, keys, (((1,), (1,)), ((), ())), preferred_element_type=F32
        ) * HD ** (-0.5)
        scores = jnp.where(causal, scores, -1e30)
        scores = jnp.exp(scores - jnp.max(scores, axis=1, keepdims=True))
        probs = (scores / jnp.sum(scores, axis=1, keepdims=True)).astype(BF16)
        heads = jnp.dot(probs, values, preferred_element_type=F32).astype(BF16)
        for h in range(4):
            att[t, SEQ * n : SEQ * (n + 1), HD * h : HD * (h + 1)] = heads[SEQ * h : SEQ * (h + 1)]
        for target in (up + tz, down + tz, beside):
            a_start(n, t, target)

    gain = gains_ref[1:]
    share = TOKENS // NT

    def l_copy(target, to):
        return pltpu.make_async_remote_copy(
            src_ref=lg.at[target], dst_ref=lg_got.at[to], send_sem=l_send.at[target], recv_sem=l_recv.at[to],
            device_id={"tp": target}, device_id_type=MESH,
        )

    def n_copy(target, to):
        return pltpu.make_async_remote_copy(
            src_ref=ssq.at[target], dst_ref=ssq_got.at[to], send_sem=n_send.at[target], recv_sem=n_recv.at[to],
            device_id={"tp": target}, device_id_type=MESH,
        )

    last = far_y + 1 - tz

    def project(n, source):
        block = jnp.concatenate([obuf[4 * source + k] for k in range(4)], axis=1)
        head[n] += jnp.dot(att[source, SEQ * n : SEQ * (n + 1)], block, preferred_element_type=F32)

    def project_most(n):
        head[n] = jnp.zeros((SEQ, FB), F32)

        def one(k, carry):
            project(n, (last + 1 + k) % NT)
            return carry

        lax.fori_loop(0, NT - 1, one, 0)

    first(0)
    o.x_forward(first=0)

    v = own_x[...]
    for k, target in x_others:
        s_copy(own_x, sum_x.at[target], 0, sx_recv.at[target], {"patch": w.block(k, 0)}).wait_recv()
        v = v + sum_x[target]
    score[pc, pz] = v
    for k, target in z_others:
        begin(s_copy(score.at[pc, pz], score.at[pc, pz], 16 + k, sg_recv.at[pz], {"patch": w.block(0, k)}))

    first(1)
    first(2)
    o.far()
    cl.x_forward(first=0)
    first(3)
    for k, target in z_others:
        s_copy(score.at[pc, target], score.at[pc, target], 0, sg_recv.at[target], {"patch": w.block(0, k)}).wait_recv()
    begin(s_copy(score.at[pc], score.at[pc], 20, s_recv.at[9], {"patch": partner}))
    second(0)
    cl.far()
    second(1)
    o.core_wait()
    project_most(0)
    second(2)
    s_copy(score.at[pc], score.at[1 - pc], 0, s_recv.at[9], {"patch": partner}).wait_recv()
    score_t[...] = jnp.transpose(score[...].reshape(SCORED, FB).astype(F32)).astype(BF16)
    project_most(1)
    second(3)
    cl.core_wait()

    gain = gains_ref[1:]
    share = TOKENS // NT

    def l_copy(target, to):
        return pltpu.make_async_remote_copy(
            src_ref=lg.at[target], dst_ref=lg_got.at[to], send_sem=l_send.at[target], recv_sem=l_recv.at[to],
            device_id={"tp": target}, device_id_type=MESH,
        )

    def n_copy(target, to):
        return pltpu.make_async_remote_copy(
            src_ref=ssq.at[target // 2], dst_ref=ssq_got.at[to], send_sem=n_send.at[target], recv_sem=n_recv.at[to],
            device_id={"tp": target}, device_id_type=MESH,
        )

    for n in range(PROMPTS):
        if n >= 2:
            project_most(n)
        third(n)
        project(n, last)

        def finish(i, carry, n=n):
            at = pl.ds(pl.multiple_of(SEQ * n + ROWS * i, ROWS), ROWS)
            local_at = pl.ds(pl.multiple_of(ROWS * i, ROWS), ROWS)
            e = early_ref[local_at, :1] > 0.5
            late = late_ref[local_at, :1] > 0.5
            v = corrupt_ref[at, :].astype(F32)
            v = jnp.where(e, cbuf[8 * n + i, 0].astype(F32), v)
            v = v + head[n, local_at, :]
            v = jnp.where(late, cbuf[8 * n + i, 1].astype(F32), v)
            squares[local_at, :] = jnp.broadcast_to(
                jnp.sum(v * v, axis=1, keepdims=True), (ROWS, 128)
            )
            fin[local_at, :] = (v * gain).astype(BF16)
            return carry

        lax.fori_loop(0, SEQ // ROWS, finish, 0)
        ssq[n] = jnp.transpose(squares[...])[:8]
        value = jnp.dot(fin[...], score_t[...], preferred_element_type=F32).astype(BF16)
        for s in range(2):
            target = 2 * n + s
            lg[target] = value[share * s : share * (s + 1)]

            @pl.when(target != t)
            def _(target=target):
                n_copy(target, t).start()
                l_copy(target, t).start()

    logits = lg[t].astype(F32)
    total = ssq[ty]
    for target in others:
        n_copy(target, target).wait_recv()
        l_copy(target, target).wait_recv()
        logits = logits + lg_got[target].astype(F32)
        total = total + ssq_got[target]
    scale = jnp.transpose(jnp.broadcast_to(lax.rsqrt(total[:1] / D + EPSILON), (SEQ, SEQ)))
    scale = jnp.where(tz == 0, scale[:share], scale[share:])
    out_ref[...] = logits * scale[:, :1]

    for target in others:
        n_copy(target, t).wait_send()
        l_copy(target, t).wait_send()

    @pl.when(swaps)
    def _():
        swap.wait_send()

    for c in started:
        c.wait_send()
    for g in (w, q, o, cl):
        g.drain()


def layer(*operands):
    vmem = pl.BlockSpec(memory_space=pltpu.VMEM)
    smem = pl.BlockSpec(memory_space=pltpu.SMEM)
    hbm = pl.BlockSpec(memory_space=pl.ANY)
    dma = pltpu.SemaphoreType.DMA
    share = TOKENS // NT
    half = SCORED // 2
    rows_dev = operands[6].shape[0]
    return pl.pallas_call(
        layer_kernel,
        out_shape=jax.ShapeDtypeStruct((share, SCORED), F32),
        in_specs=[hbm] * 7 + [smem] + [vmem] * 5,
        out_specs=vmem,
        scratch_shapes=[
            pltpu.VMEM((TOKENS, FB), BF16),
            pltpu.VMEM((2, ROWS, FB), BF16),
            pltpu.VMEM((128, WCOLS), BF16),
            pltpu.VMEM((FB, 128), BF16),
            pltpu.VMEM((FB, 128), BF16),
            pltpu.VMEM((rows_dev, D), BF16),
            pltpu.VMEM((3 * ROWS, FB), BF16),
            pltpu.VMEM((NT, 3 * ROWS, FB), BF16),
            pltpu.VMEM((NP, 2 * ROWS, 128), BF16),
            pltpu.VMEM((NP, 128, WCOLS), BF16),
            pltpu.VMEM((2 * ROWS, WCOLS), F32),
            pltpu.VMEM((2, ROWS, WCOLS), BF16),
            pltpu.VMEM((NP, 2, ROWS, WCOLS), BF16),
            pltpu.VMEM((NP, FB, 128), BF16),
            pltpu.VMEM((NP, 2, ROWS, FB), BF16),
            pltpu.VMEM((NT, TOKENS, FB), BF16),
            pltpu.VMEM((PROMPTS, SEQ, FB), F32),
            pltpu.VMEM((SEQ, SEQ), F32),
            pltpu.VMEM((SEQ, SEQ), F32),
            pltpu.VMEM((NT, SCORED, FB), BF16),
            pltpu.VMEM((NT, half, FB), BF16),
            pltpu.VMEM((4, 2, half, FB), BF16),
            pltpu.VMEM((4, 2, half, FB), BF16),
            pltpu.VMEM((2, half, FB), BF16),
            pltpu.VMEM((half, FB), BF16),
            pltpu.VMEM((4, half // 4, FB), BF16),
            pltpu.VMEM((4, half // 4, FB), BF16),
            pltpu.VMEM((4, half // 4, FB), BF16),
            pltpu.VMEM((half // 4, FB), BF16),
            pltpu.VMEM((2, 4, half // 4, FB), BF16),
            pltpu.VMEM((SEQ, FB), BF16),
            pltpu.VMEM((FB, SCORED), BF16),
            pltpu.VMEM((SEQ, 128), F32),
            pltpu.VMEM((PROMPTS, 8, 128), F32),
            pltpu.VMEM((NT, 8, 128), F32),
            pltpu.VMEM((NT, share, SCORED), BF16),
            pltpu.VMEM((NT, share, SCORED), BF16),
            dma((7,)),
            dma((NT,)), dma((NT,)),
            dma((N_SENDS,)), dma((NP,)),
            dma((N_SENDS,)), dma((NP,)),
            dma((N_SENDS,)), dma((NP,)),
            dma((N_SENDS,)), dma((NP,)),
            dma((32,)), dma((NT, PROMPTS)),
            dma((22,)), dma((11,)), dma((4,)), dma((4,)), dma((4,)),
            dma((NT,)), dma((NT,)), dma((NT,)), dma((NT,)),
        ],
        compiler_params=pltpu.CompilerParams(
            collective_id=0, has_side_effects=True, vmem_limit_bytes=60 * 1024 * 1024
        ),
        cost_estimate=pl.CostEstimate(
            flops=4 * 10**9, bytes_accessed=20 * 2**20, transcendentals=10**6
        ),
        name="layer",
    )(*operands)


def rope_tables():
    half = HD // 2
    exponents = -(np.arange(half, dtype=np.float32) * np.float32(2.0 / HD))
    freqs = (np.float32(THETA) ** exponents).astype(np.float32)
    angles = np.arange(SEQ, dtype=np.float32)[:, None] * freqs[None, :]
    cosine, sine = np.cos(angles), np.sin(angles)
    return (
        np.concatenate([cosine, cosine], axis=1).astype(np.float32),
        np.concatenate([-sine, sine], axis=1).astype(np.float32),
    )


def on_device(
    resid_corrupt, resid_clean, patch_level, patch_mask, norm_gain, final_gain,
    w_query, w_key, w_value, w_out, unembed, scored_ids, base_logits,
):
    cosine, sine = rope_tables()
    gains = jnp.stack([norm_gain, final_gain]).astype(F32)
    out = layer(
        resid_corrupt, resid_clean, w_query, w_key, w_value, w_out, unembed,
        patch_level, patch_mask, scored_ids[None, :], gains, jnp.asarray(cosine), jnp.asarray(sine),
    )
    return (out - base_logits)[None]


def solution(mesh):
    placed = (
        P(None, "tp"),
        P(None, "patch", "tp"),
        P("patch"),
        P("patch", None),
        P("tp"),
        P("tp"),
        P("patch", "tp"),
        P("patch", "tp"),
        P("patch", "tp"),
        P("tp", "patch"),
        P(("patch", "tp"), None),
        P(),
        P("tp", None),
    )
    return jax.shard_map(
        on_device, mesh=mesh, in_specs=placed, out_specs=P("patch", "tp", None), check_vma=False
    )
```

```python
import jax
import jax.numpy as jnp
import numpy as np
from jax import lax
from jax.experimental import pallas as pl
from jax.experimental.pallas import tpu as pltpu
from jax.sharding import PartitionSpec as P

D = 4096
HD = 128
SEQ = 128
PROMPTS = 4
TOKENS = PROMPTS * SEQ
SCORED = 256
NP = 32
NT = 8
FB = D // NT
ROWS = TOKENS // NP
QCOLS = 512
KVCOL = 128
WCOLS = QCOLS + 2 * KVCOL
EPSILON = 1e-05
THETA = 500000.0
MESH = pl.DeviceIdType.MESH
F32 = jnp.float32
BF16 = jnp.bfloat16
N_SENDS = 31


class PatchGather:
    def __init__(self, own, buf, send, recv):
        self.own, self.buf, self.send, self.recv = own, buf, send, recv
        me = lax.axis_index("patch")
        self.me = me
        self.x, self.z, self.c = me // 8, (me // 2) % 4, me % 2
        self.way = 1 - 2 * self.c
        self.started = []

    def block(self, dx, dz, other=False):
        c = 1 - self.c if other else self.c
        return ((self.x + dx) % 4) * 8 + ((self.z + dz + 4) % 4) * 2 + c

    def copy(self, src, index, target, slot):
        return pltpu.make_async_remote_copy(
            src_ref=src,
            dst_ref=self.buf.at[index],
            send_sem=self.send.at[slot],
            recv_sem=self.recv.at[index],
            device_id={"patch": target},
            device_id_type=MESH,
        )

    def start(self, src, index, target):
        c = self.copy(src, index, target, len(self.started))
        c.start()
        self.started.append(c)

    def wait(self, index):
        self.copy(self.buf.at[index], index, self.block(1, 0), 0).wait_recv()

    def z_send(self):
        for dz in (self.way, -self.way):
            self.start(self.own, self.me, self.block(0, dz))

    def own_send(self):
        for target in (self.block(1, 0), self.block(3, 0), self.block(0, 0, True)):
            self.start(self.own, self.me, target)

    def z_relay(self):
        b = self.block(0, -self.way)
        self.wait(b)
        self.start(self.buf.at[b], b, self.block(0, self.way))

    def spread(self, b):
        for target in (self.block(1, 0), self.block(3, 0), self.block(0, 0, True)):
            self.start(self.buf.at[b], b, target)

    def z_forward(self, relayed=False):
        if not relayed:
            self.z_relay()
        for k, dz in enumerate((-self.way, self.way, 2)):
            b = self.block(0, dz)
            if k > 0:
                self.wait(b)
            self.spread(b)

    def x_near(self, k, then=None):
        for dx in (3, 1):
            b = self.block(dx, (0, -self.way, self.way, 2)[k])
            self.wait(b)
            if (k in (0, 3)) == (dx == 3):
                self.start(self.buf.at[b], b, self.block(4 - dx, 0))
            self.start(self.buf.at[b], b, self.block(0, 0, True))
            if then is not None:
                then(b)

    def x_forward(self, then=None, first=1):
        for k in range(first, 4):
            self.x_near(k, then)

    def far(self, then=None):
        for dz in (0, -self.way, self.way, 2):
            b = self.block(2, dz)
            self.wait(b)
            self.start(self.buf.at[b], b, self.block(0, 0, True))
            if then is not None:
                then(b)

    def core_wait(self, then=None, steps=(0, 3, 1, 2)):
        for dx in steps:
            for dz in (0, self.way, -self.way, 2):
                b = self.block(dx, dz, True)
                self.wait(b)
                if then is not None:
                    then(b)

    def drain(self):
        for c in self.started:
            c.wait_send()


def layer_kernel(
    corrupt_hbm, clean_hbm, wq_hbm, wk_hbm, wv_hbm, wo_hbm, unembed_hbm,
    level_ref, mask_ref, ids_ref, ngain_ref, fgain_ref, cos_ref, sin_ref,
    out_ref,
    corrupt_ref, clean_ref, w_ref, wo_ref, wo_own, unembed_ref,
    xin, xrecv, nbuf, wbuf, acc, qown, qbuf, obuf, cbuf, att, head, early_ref, late_ref,
    chosen, chosen_got, paired, spread, mine, mine_got, spread_z, sum_z, sum_x, own_x, score, fin, score_t, squares, ssq, ssq_got, lg, lg_got,
    local, x_send, x_recv, w_send, w_recv, q_send, q_recv, o_send, o_recv, c_send, c_recv, a_send, a_recv,
    s_send, s_recv, sz_recv, sx_recv, sg_recv, l_send, l_recv, n_send, n_recv,
):
    t = lax.axis_index("tp")
    w = PatchGather(w_ref, wbuf, w_send, w_recv)
    q = PatchGather(qown, qbuf, q_send, q_recv)
    o = PatchGather(wo_own, obuf, o_send, o_recv)
    cl = PatchGather(clean_ref, cbuf, c_send, c_recv)
    me, px, pz, pc = w.me, w.x, w.z, w.c
    ty, tz = t // 2, t % 2
    beside = t + 1 - 2 * tz
    others = [(t + k) % NT for k in range(1, NT)]
    z_others = [(k, (pz + k) % 4) for k in (1, 3, 2)]
    x_others = [(k, (px + k) % 4) for k in (1, 3, 2)]
    partner = w.block(0, 0, True)
    swap_p, swap_t = 4 * t + me % 4, me // 4
    swaps = swap_t != t

    loads = [
        pltpu.make_async_copy(src, dst, local.at[k])
        for k, (src, dst) in enumerate(
            [
                (corrupt_hbm, corrupt_ref),
                (clean_hbm, clean_ref),
                (wq_hbm, w_ref.at[:, pl.ds(0, QCOLS)]),
                (wk_hbm, w_ref.at[:, pl.ds(QCOLS, KVCOL)]),
                (wv_hbm, w_ref.at[:, pl.ds(QCOLS + KVCOL, KVCOL)]),
                (wo_hbm, wo_ref),
                (unembed_hbm, unembed_ref),
            ]
        )
    ]
    for c in loads:
        c.start()
    barrier = pltpu.get_barrier_semaphore()
    peers = (
        [{"tp": k} for k in others]
        + [{"patch": w.block(0, dz)} for dz in (1, 3, 2)]
        + [{"patch": w.block(dx, 0)} for dx in (1, 3, 2)]
        + [{"patch": partner}]
    )
    for peer in peers:
        pl.semaphore_signal(barrier, inc=1, device_id=peer, device_id_type=MESH)

    @pl.when(swaps)
    def _():
        pl.semaphore_signal(
            barrier, inc=1, device_id={"patch": swap_p, "tp": swap_t}, device_id_type=MESH
        )

    for c in loads[:2]:
        c.wait()
    xin[:ROWS] = corrupt_ref[pl.ds(pl.multiple_of(me * ROWS, ROWS), ROWS), :]
    xin[ROWS : 2 * ROWS] = clean_ref[0]
    xin[2 * ROWS :] = jnp.broadcast_to(ngain_ref[...].astype(F32).reshape(1, FB), (ROWS, FB)).astype(BF16)
    xrecv[t] = xin[...]
    spliced = jnp.transpose(jnp.broadcast_to(mask_ref[...].astype(F32), (SEQ, SEQ)))
    level = level_ref[0].astype(F32)
    early_ref[...] = spliced * (1.0 - level)
    late_ref[...] = spliced * level
    cbuf[me] = clean_ref[...]
    for c in loads[2:6]:
        c.wait()
    pl.semaphore_wait(barrier, len(peers) + swaps.astype(jnp.int32))

    started = []

    def begin(c):
        c.start()
        started.append(c)

    def x_copy(k, target, to):
        return pltpu.make_async_remote_copy(
            src_ref=xin, dst_ref=xrecv.at[to], send_sem=x_send.at[k], recv_sem=x_recv.at[to],
            device_id={"tp": target}, device_id_type=MESH,
        )

    def s_copy(src, dst, send, recv, where):
        return pltpu.make_async_remote_copy(
            src_ref=src, dst_ref=dst, send_sem=s_send.at[send], recv_sem=recv,
            device_id=where, device_id_type=MESH,
        )

    w.z_send()
    w.own_send()
    for k, target in enumerate(others):
        begin(x_copy(k, target, t))
    swap = s_copy(wo_ref, wo_own, 21, s_recv.at[10], {"patch": swap_p, "tp": swap_t})

    @pl.when(swaps)
    def _():
        swap.start()

    loads[6].wait()
    rows_dev = unembed_ref.shape[0]
    wanted = jnp.transpose(jnp.broadcast_to(ids_ref[...].astype(F32), (SCORED, SCORED)))[:, :1]
    wanted = wanted.astype(jnp.int32) - (me * NT + t) * rows_dev
    owned = jnp.where(
        wanted == lax.broadcasted_iota(jnp.int32, (SCORED, rows_dev), 1), 1.0, 0.0
    ).astype(BF16)
    for k in range(NT):
        chosen[k] = jnp.dot(
            owned, unembed_ref[:, FB * k : FB * (k + 1)], preferred_element_type=F32
        ).astype(BF16)
    half = SCORED // 2
    pair = s_copy(
        chosen.at[:, pl.ds(pl.multiple_of(half * (1 - pc), half), half)],
        chosen_got, 0, s_recv.at[0], {"patch": partner},
    )
    begin(pair)
    pair.wait_recv()
    paired[...] = (
        chosen[:, pl.ds(pl.multiple_of(half * pc, half), half)] + chosen_got[...]
    ).reshape(4, 2, half, FB)
    y_others = [(k, (ty + k) % 4) for k in (1, 3, 2)]
    for k, y in y_others:
        begin(s_copy(paired.at[y], spread.at[ty], k, s_recv.at[1 + ty], {"tp": 2 * y + tz}))

    w.x_near(0)
    w.z_forward()

    @pl.when(swaps)
    def _():
        swap.wait_recv()

    @pl.when(jnp.logical_not(swaps))
    def _():
        wo_own[...] = wo_ref[...]

    o.z_send()
    for target in others:
        x_copy(0, target, target).wait_recv()
    total = jnp.zeros((2 * ROWS, 1), F32)
    for k in range(NT):
        v = xrecv[k, : 2 * ROWS, :].astype(F32)
        total = total + jnp.sum(v * v, axis=1, keepdims=True)
    scale = lax.rsqrt(total / D + EPSILON)
    for k in range(NT):
        v = xrecv[k, : 2 * ROWS, :].astype(F32)
        g = xrecv[k, 2 * ROWS :, :].astype(F32)[:1]
        v = (v * scale * g).astype(BF16)
        for j in range(4):
            nbuf[4 * k + j] = v[:, 128 * j : 128 * (j + 1)]

    v = paired[ty]
    for k, y in y_others:
        s_copy(paired.at[y], spread.at[y], 0, s_recv.at[1 + y], {"tp": 2 * y + tz}).wait_recv()
        v = v + spread[y]
    mine[...] = v
    begin(s_copy(mine.at[1 - tz], mine_got, 4, s_recv.at[5], {"tp": beside}))

    acc[...] = jnp.dot(nbuf[me], w_ref[...], preferred_element_type=F32)

    def add(b):
        acc[...] += jnp.dot(nbuf[b], wbuf[b], preferred_element_type=F32)

    for b in [w.block(0, dz) for dz in (3, 1, 2)] + [w.block(dx, 0) for dx in (3, 1)]:
        add(b)
    w.x_forward(add)
    obuf[me] = wo_own[...]
    o.z_relay()
    cl.z_send()

    s_copy(mine.at[1 - tz], mine_got, 4, s_recv.at[5], {"tp": beside}).wait_recv()
    spread_z[...] = (mine[tz] + mine_got[...]).reshape(4, half // 4, FB)
    for k, target in z_others:
        begin(s_copy(spread_z.at[target], sum_z.at[pz], 8 + k, sz_recv.at[pz], {"patch": w.block(0, k)}))

    w.far(add)
    w.core_wait(add)

    at = pl.ds(pl.multiple_of((me * ROWS) % SEQ, ROWS), ROWS)
    cosine = jnp.concatenate([cos_ref[at, :]] * 2, axis=0)
    sine = jnp.concatenate([sin_ref[at, :]] * 2, axis=0)
    for h in range(WCOLS // HD):
        v = acc[:, HD * h : HD * (h + 1)]
        if h < 5:
            v = v * cosine + pltpu.roll(v, HD // 2, 1) * sine
        v = v.astype(BF16)
        for s in range(2):
            qown[s, :, HD * h : HD * (h + 1)] = v[ROWS * s : ROWS * (s + 1)]
    qbuf[me] = qown[...]
    q.z_send()
    q.own_send()

    early = early_ref[...] > 0.5
    row = lax.broadcasted_iota(jnp.int32, (4 * SEQ, SEQ), 0) % SEQ
    col = lax.broadcasted_iota(jnp.int32, (4 * SEQ, SEQ), 1)
    causal = row >= col

    def a_copy(index, n, source, target):
        rows = pl.ds(SEQ * n, SEQ)
        return pltpu.make_async_remote_copy(
            src_ref=att.at[source, rows], dst_ref=att.at[source, rows],
            send_sem=a_send.at[index], recv_sem=a_recv.at[source, n],
            device_id={"tp": target}, device_id_type=MESH,
        )

    a_count = []

    def a_start(n, source, target):
        begin(a_copy(len(a_count), n, source, target))
        a_count.append(n)

    def a_wait(n, source):
        a_copy(0, n, source, others[0]).wait_recv()

    up, down, far_y = ((ty + 1) % 4) * 2, ((ty + 3) % 4) * 2, ((ty + 2) % 4) * 2
    near = (down, up)

    def across(n):
        return n < 2

    def clockwise(n):
        return n % 2 == 0

    def first(n):
        for y in near:
            a_wait(n, y + tz)
            if clockwise(n) == (y is down):
                a_start(n, y + tz, (up if y is down else down) + tz)
            if across(n):
                a_start(n, y + tz, beside)
        a_wait(n, beside)
        if not across(n):
            a_start(n, beside, up + tz)
            a_start(n, beside, down + tz)

    def second(n):
        a_wait(n, far_y + tz)
        if across(n):
            a_start(n, far_y + tz, beside)

    def crossed(n):
        for y in near:
            a_wait(n, y + 1 - tz)
            if not across(n) and clockwise(n) == (y is down):
                a_start(n, y + 1 - tz, (up if y is down else down) + tz)

    def third(n):
        a_wait(n, far_y + 1 - tz)

    prompts = [(px + dx) % 4 for dx in (0, 3, 1, 2)]

    def attend(n):
        prompt = prompts[n]

        def picked(lo, hi):
            a = qbuf[pl.ds(8 * prompt, 8), 0, :, lo:hi].reshape(SEQ, hi - lo).astype(F32)
            b = qbuf[pl.ds(8 * prompt, 8), 1, :, lo:hi].reshape(SEQ, hi - lo).astype(F32)
            return jnp.where(early, b, a).astype(BF16)

        queries = jnp.concatenate([picked(HD * h, HD * (h + 1)) for h in range(4)], axis=0)
        keys = picked(QCOLS, QCOLS + HD)
        values = picked(QCOLS + HD, QCOLS + 2 * HD)
        scores = lax.dot_general(
            queries, keys, (((1,), (1,)), ((), ())), preferred_element_type=F32
        ) * HD ** (-0.5)
        scores = jnp.where(causal, scores, -1e30)
        scores = jnp.exp(scores - jnp.max(scores, axis=1, keepdims=True))
        probs = (scores / jnp.sum(scores, axis=1, keepdims=True)).astype(BF16)
        heads = jnp.dot(probs, values, preferred_element_type=F32).astype(BF16)
        for h in range(4):
            att[t, SEQ * n : SEQ * (n + 1), HD * h : HD * (h + 1)] = heads[SEQ * h : SEQ * (h + 1)]
        for target in (up + tz, down + tz, beside):
            a_start(n, t, target)

    q.z_forward()
    q.x_near(0)
    q.core_wait(steps=(0,))
    attend(0)

    v = spread_z[pz]
    for k, target in z_others:
        s_copy(spread_z.at[target], sum_z.at[target], 0, sz_recv.at[target], {"patch": w.block(0, k)}).wait_recv()
        v = v + sum_z[target]
    own_x[...] = v
    for k, target in x_others:
        begin(s_copy(own_x, sum_x.at[px], 12 + k, sx_recv.at[px], {"patch": w.block(k, 0)}))


    q.x_forward()
    cl.z_relay()
    o.own_send()
    o.z_forward(True)
    q.core_wait(steps=(3, 1))
    attend(1)
    attend(2)

    v = own_x[...]
    for k, target in x_others:
        s_copy(own_x, sum_x.at[target], 0, sx_recv.at[target], {"patch": w.block(k, 0)}).wait_recv()
        v = v + sum_x[target]
    score[pc, pz] = v
    for k, target in z_others:
        begin(s_copy(score.at[pc, pz], score.at[pc, pz], 16 + k, sg_recv.at[pz], {"patch": w.block(0, k)}))

    first(0)
    cl.own_send()
    cl.z_forward(True)
    q.far()
    q.core_wait(steps=(2,))
    attend(3)


    last = far_y + 1 - tz

    def project(n, count, sources, fresh=False):
        rows = pl.ds(SEQ * n, SEQ * count)
        for k, source in enumerate(sources):
            block = jnp.concatenate([obuf[4 * source + j] for j in range(4)], axis=1)
            piece = jnp.dot(att[source, rows], block, preferred_element_type=F32)
            if fresh and k == 0:
                head[rows] = piece
            else:
                head[rows] += piece

    first(1)
    first(2)
    o.x_near(0)
    o.x_near(1)
    second(0)

    o.x_near(2)
    o.x_near(3)
    first(3)
    for k, target in z_others:
        s_copy(score.at[pc, target], score.at[pc, target], 0, sg_recv.at[target], {"patch": w.block(0, k)}).wait_recv()
    begin(s_copy(score.at[pc], score.at[pc], 20, s_recv.at[9], {"patch": partner}))
    second(1)
    crossed(2)
    cl.x_forward(first=0)

    o.far()
    crossed(3)
    o.core_wait()
    project(0, 4, (t, beside, up + tz, down + tz), True)
    cl.far()
    crossed(0)
    crossed(1)
    second(2)
    second(3)
    project(0, 4, (far_y + tz, up + 1 - tz, down + 1 - tz))
    s_copy(score.at[pc], score.at[1 - pc], 0, s_recv.at[9], {"patch": partner}).wait_recv()
    score_t[...] = jnp.transpose(score[...].reshape(SCORED, FB).astype(F32)).astype(BF16)
    cl.core_wait()

    gain = fgain_ref[...].astype(F32).reshape(1, FB)
    share = TOKENS // NT

    def l_copy(target, to):
        return pltpu.make_async_remote_copy(
            src_ref=lg.at[target], dst_ref=lg_got.at[to], send_sem=l_send.at[target], recv_sem=l_recv.at[to],
            device_id={"tp": target}, device_id_type=MESH,
        )

    def n_copy(target, to):
        return pltpu.make_async_remote_copy(
            src_ref=ssq.at[target // 2], dst_ref=ssq_got.at[to], send_sem=n_send.at[target], recv_sem=n_recv.at[to],
            device_id={"tp": target}, device_id_type=MESH,
        )

    for n in range(PROMPTS):
        if n == 0:
            third(0)
            third(1)
            project(0, 2, (last,))
        if n == 2:
            third(2)
            third(3)
            project(2, 2, (last,))

        def finish(i, carry, n=n):
            at = pl.ds(pl.multiple_of(SEQ * n + ROWS * i, ROWS), ROWS)
            token = pl.ds(pl.multiple_of(SEQ * prompts[n] + ROWS * i, ROWS), ROWS)
            local_at = pl.ds(pl.multiple_of(ROWS * i, ROWS), ROWS)
            e = early_ref[local_at, :1] > 0.5
            late = late_ref[local_at, :1] > 0.5
            v = corrupt_ref[token, :].astype(F32)
            v = jnp.where(e, cbuf[8 * prompts[n] + i, 0].astype(F32), v)
            v = v + head[at, :]
            v = jnp.where(late, cbuf[8 * prompts[n] + i, 1].astype(F32), v)
            squares[local_at, :] = jnp.broadcast_to(
                jnp.sum(v * v, axis=1, keepdims=True), (ROWS, 128)
            )
            fin[local_at, :] = (v * gain).astype(BF16)
            return carry

        lax.fori_loop(0, SEQ // ROWS, finish, 0, unroll=4)
        ssq[prompts[n]] = jnp.transpose(squares[...])[:8]
        value = jnp.dot(fin[...], score_t[...], preferred_element_type=F32).astype(BF16)
        for s in range(2):
            target = 2 * prompts[n] + s
            lg[target] = value[share * s : share * (s + 1)]

            @pl.when(target != t)
            def _(target=target):
                n_copy(target, t).start()
                l_copy(target, t).start()

    logits = lg[t].astype(F32)
    total = ssq[ty]
    for target in others:
        n_copy(target, target).wait_recv()
        l_copy(target, target).wait_recv()
        logits = logits + lg_got[target].astype(F32)
        total = total + ssq_got[target]
    scale = jnp.transpose(jnp.broadcast_to(lax.rsqrt(total[:1] / D + EPSILON), (SEQ, SEQ)))
    scale = jnp.where(tz == 0, scale[:share], scale[share:])
    out_ref[...] = logits * scale[:, :1]

    for target in others:
        n_copy(target, t).wait_send()
        l_copy(target, t).wait_send()

    @pl.when(swaps)
    def _():
        swap.wait_send()

    for c in started:
        c.wait_send()
    for g in (w, q, o, cl):
        g.drain()


def layer(*operands):
    vmem = pl.BlockSpec(memory_space=pltpu.VMEM)
    smem = pl.BlockSpec(memory_space=pltpu.SMEM)
    hbm = pl.BlockSpec(memory_space=pl.ANY)
    dma = pltpu.SemaphoreType.DMA
    share = TOKENS // NT
    half = SCORED // 2
    rows_dev = operands[6].shape[0]
    return pl.pallas_call(
        layer_kernel,
        out_shape=jax.ShapeDtypeStruct((share, SCORED), F32),
        in_specs=[hbm] * 7 + [smem] + [vmem] * 6,
        out_specs=vmem,
        scratch_shapes=[
            pltpu.VMEM((TOKENS, FB), BF16),
            pltpu.VMEM((2, ROWS, FB), BF16),
            pltpu.VMEM((128, WCOLS), BF16),
            pltpu.VMEM((FB, 128), BF16),
            pltpu.VMEM((FB, 128), BF16),
            pltpu.VMEM((rows_dev, D), BF16),
            pltpu.VMEM((3 * ROWS, FB), BF16),
            pltpu.VMEM((NT, 3 * ROWS, FB), BF16),
            pltpu.VMEM((NP, 2 * ROWS, 128), BF16),
            pltpu.VMEM((NP, 128, WCOLS), BF16),
            pltpu.VMEM((2 * ROWS, WCOLS), F32),
            pltpu.VMEM((2, ROWS, WCOLS), BF16),
            pltpu.VMEM((NP, 2, ROWS, WCOLS), BF16),
            pltpu.VMEM((NP, FB, 128), BF16),
            pltpu.VMEM((NP, 2, ROWS, FB), BF16),
            pltpu.VMEM((NT, TOKENS, FB), BF16),
            pltpu.VMEM((TOKENS, FB), F32),
            pltpu.VMEM((SEQ, SEQ), F32),
            pltpu.VMEM((SEQ, SEQ), F32),
            pltpu.VMEM((NT, SCORED, FB), BF16),
            pltpu.VMEM((NT, half, FB), BF16),
            pltpu.VMEM((4, 2, half, FB), BF16),
            pltpu.VMEM((4, 2, half, FB), BF16),
            pltpu.VMEM((2, half, FB), BF16),
            pltpu.VMEM((half, FB), BF16),
            pltpu.VMEM((4, half // 4, FB), BF16),
            pltpu.VMEM((4, half // 4, FB), BF16),
            pltpu.VMEM((4, half // 4, FB), BF16),
            pltpu.VMEM((half // 4, FB), BF16),
            pltpu.VMEM((2, 4, half // 4, FB), BF16),
            pltpu.VMEM((SEQ, FB), BF16),
            pltpu.VMEM((FB, SCORED), BF16),
            pltpu.VMEM((SEQ, 128), F32),
            pltpu.VMEM((PROMPTS, 8, 128), F32),
            pltpu.VMEM((NT, 8, 128), F32),
            pltpu.VMEM((NT, share, SCORED), BF16),
            pltpu.VMEM((NT, share, SCORED), BF16),
            dma((7,)),
            dma((NT,)), dma((NT,)),
            dma((N_SENDS,)), dma((NP,)),
            dma((N_SENDS,)), dma((NP,)),
            dma((N_SENDS,)), dma((NP,)),
            dma((N_SENDS,)), dma((NP,)),
            dma((32,)), dma((NT, PROMPTS)),
            dma((22,)), dma((11,)), dma((4,)), dma((4,)), dma((4,)),
            dma((NT,)), dma((NT,)), dma((NT,)), dma((NT,)),
        ],
        compiler_params=pltpu.CompilerParams(
            collective_id=0, has_side_effects=True, vmem_limit_bytes=60 * 1024 * 1024
        ),
        cost_estimate=pl.CostEstimate(
            flops=4 * 10**9, bytes_accessed=20 * 2**20, transcendentals=10**6
        ),
        name="layer",
    )(*operands)


def rope_tables():
    half = HD // 2
    exponents = -(np.arange(half, dtype=np.float32) * np.float32(2.0 / HD))
    freqs = (np.float32(THETA) ** exponents).astype(np.float32)
    angles = np.arange(SEQ, dtype=np.float32)[:, None] * freqs[None, :]
    cosine, sine = np.cos(angles), np.sin(angles)
    return (
        np.concatenate([cosine, cosine], axis=1).astype(np.float32),
        np.concatenate([-sine, sine], axis=1).astype(np.float32),
    )


def on_device(
    resid_corrupt, resid_clean, patch_level, patch_mask, norm_gain, final_gain,
    w_query, w_key, w_value, w_out, unembed, scored_ids, base_logits,
):
    cosine, sine = rope_tables()
    out = layer(
        resid_corrupt, resid_clean, w_query, w_key, w_value, w_out, unembed,
        patch_level, patch_mask, scored_ids[None, :], norm_gain, final_gain, jnp.asarray(cosine), jnp.asarray(sine),
    )
    return (out - base_logits)[None]


def solution(mesh):
    placed = (
        P(None, "tp"),
        P(None, "patch", "tp"),
        P("patch"),
        P("patch", None),
        P("tp"),
        P("tp"),
        P("patch", "tp"),
        P("patch", "tp"),
        P("patch", "tp"),
        P("tp", "patch"),
        P(("patch", "tp"), None),
        P(),
        P("tp", None),
    )
    return jax.shard_map(
        on_device, mesh=mesh, in_specs=placed, out_specs=P("patch", "tp", None), check_vma=False
    )
```

```python
import jax
import jax.numpy as jnp
import numpy as np
from jax import lax
from jax.experimental import pallas as pl
from jax.experimental.pallas import tpu as pltpu
from jax.sharding import PartitionSpec as P

D = 4096
HD = 128
SEQ = 128
PROMPTS = 4
TOKENS = PROMPTS * SEQ
SCORED = 256
NP = 32
NT = 8
FB = D // NT
ROWS = TOKENS // NP
QCOLS = 512
KVCOL = 128
WCOLS = QCOLS + 2 * KVCOL
EPSILON = 1e-05
THETA = 500000.0
MESH = pl.DeviceIdType.MESH
F32 = jnp.float32
BF16 = jnp.bfloat16
N_SENDS = 31


class PatchGather:
    def __init__(self, own, buf, send, recv):
        self.own, self.buf, self.send, self.recv = own, buf, send, recv
        me = lax.axis_index("patch")
        self.me = me
        self.x, self.z, self.c = me // 8, (me // 2) % 4, me % 2
        self.way = 1 - 2 * self.c
        self.started = []

    def block(self, dx, dz, other=False):
        c = 1 - self.c if other else self.c
        return ((self.x + dx) % 4) * 8 + ((self.z + dz + 4) % 4) * 2 + c

    def copy(self, src, index, target, slot):
        return pltpu.make_async_remote_copy(
            src_ref=src,
            dst_ref=self.buf.at[index],
            send_sem=self.send.at[slot],
            recv_sem=self.recv.at[index],
            device_id={"patch": target},
            device_id_type=MESH,
        )

    def start(self, src, index, target):
        c = self.copy(src, index, target, len(self.started))
        c.start()
        self.started.append(c)

    def wait(self, index):
        self.copy(self.buf.at[index], index, self.block(1, 0), 0).wait_recv()

    def z_send(self):
        for dz in (self.way, -self.way):
            self.start(self.own, self.me, self.block(0, dz))

    def own_send(self):
        for target in (self.block(1, 0), self.block(3, 0), self.block(0, 0, True)):
            self.start(self.own, self.me, target)

    def z_relay(self):
        b = self.block(0, -self.way)
        self.wait(b)
        self.start(self.buf.at[b], b, self.block(0, self.way))

    def spread(self, b):
        for target in (self.block(1, 0), self.block(3, 0), self.block(0, 0, True)):
            self.start(self.buf.at[b], b, target)

    def z_forward(self, relayed=False):
        if not relayed:
            self.z_relay()
        for k, dz in enumerate((-self.way, self.way, 2)):
            b = self.block(0, dz)
            if k > 0:
                self.wait(b)
            self.spread(b)

    def x_near(self, k, then=None):
        for dx in (3, 1):
            b = self.block(dx, (0, -self.way, self.way, 2)[k])
            self.wait(b)
            if (k in (0, 3)) == (dx == 3):
                self.start(self.buf.at[b], b, self.block(4 - dx, 0))
            self.start(self.buf.at[b], b, self.block(0, 0, True))
            if then is not None:
                then(b)

    def x_forward(self, then=None, first=1):
        for k in range(first, 4):
            self.x_near(k, then)

    def far(self, then=None):
        for dz in (0, -self.way, self.way, 2):
            b = self.block(2, dz)
            self.wait(b)
            self.start(self.buf.at[b], b, self.block(0, 0, True))
            if then is not None:
                then(b)

    def core_wait(self, then=None, steps=(0, 3, 1, 2)):
        for dx in steps:
            for dz in (0, self.way, -self.way, 2):
                b = self.block(dx, dz, True)
                self.wait(b)
                if then is not None:
                    then(b)

    def drain(self):
        for c in self.started:
            c.wait_send()


def layer_kernel(
    corrupt_hbm, clean_hbm, wq_hbm, wk_hbm, wv_hbm, wo_hbm, unembed_hbm,
    level_ref, mask_ref, ids_ref, ngain_ref, fgain_ref, cos_ref, sin_ref,
    out_ref,
    corrupt_ref, clean_ref, wo_ref, wo_own, unembed_ref,
    x_own, x_sum, x_got, nsend, ngot, wbuf, acc, pbuf, pgot, qown, qbuf, obuf, cbuf, att, head, early_ref, late_ref,
    chosen, chosen_got, paired, spread, mine, mine_got, spread_z, sum_z, sum_x, own_x, score, fin, score_t, squares, ssq, ssq_got, lg, lg_got,
    local, x_send, x_recv, v_send, v_recv, p_send, p_recv, w_send, w_recv, q_send, q_recv, o_send, o_recv, c_send, c_recv, a_send, a_recv,
    s_send, s_recv, sz_recv, sx_recv, sg_recv, l_send, l_recv, n_send, n_recv,
):
    t = lax.axis_index("tp")
    q = PatchGather(qown, qbuf, q_send, q_recv)
    o = PatchGather(wo_own, obuf, o_send, o_recv)
    cl = PatchGather(clean_ref, cbuf, c_send, c_recv)
    w = q
    me, px, pz, pc = w.me, w.x, w.z, w.c
    ty, tz = t // 2, t % 2
    beside = t + 1 - 2 * tz
    others = [(t + k) % NT for k in range(1, NT)]
    z_others = [(k, (pz + k) % 4) for k in (1, 3, 2)]
    x_others = [(k, (px + k) % 4) for k in (1, 3, 2)]
    partner = w.block(0, 0, True)
    swap_p, swap_t = 4 * t + me % 4, me // 4
    swaps = swap_t != t

    loads = [
        pltpu.make_async_copy(src, dst, local.at[k])
        for k, (src, dst) in enumerate(
            [
                (corrupt_hbm, corrupt_ref),
                (clean_hbm, clean_ref),
                (wq_hbm, wbuf.at[2 * px + pc, :, pl.ds(0, QCOLS)]),
                (wk_hbm, wbuf.at[2 * px + pc, :, pl.ds(QCOLS, KVCOL)]),
                (wv_hbm, wbuf.at[2 * px + pc, :, pl.ds(QCOLS + KVCOL, KVCOL)]),
                (wo_hbm, wo_ref),
                (unembed_hbm, unembed_ref),
            ]
        )
    ]
    for c in loads:
        c.start()
    barrier = pltpu.get_barrier_semaphore()
    peers = (
        [{"tp": k} for k in others]
        + [{"patch": w.block(0, dz)} for dz in (1, 3, 2)]
        + [{"patch": w.block(dx, 0)} for dx in (1, 3, 2)]
        + [{"patch": partner}]
        + [{"patch": w.block(0, dz), "tp": k} for dz in (1, 3, 2) for k in others]
    )
    for peer in peers:
        pl.semaphore_signal(barrier, inc=1, device_id=peer, device_id_type=MESH)

    @pl.when(swaps)
    def _():
        pl.semaphore_signal(
            barrier, inc=1, device_id={"patch": swap_p, "tp": swap_t}, device_id_type=MESH
        )

    for c in loads[:2]:
        c.wait()
    x_own[:ROWS] = corrupt_ref[pl.ds(pl.multiple_of(me * ROWS, ROWS), ROWS), :].astype(F32)
    x_own[ROWS:] = clean_ref[0].astype(F32)
    v = x_own[...]
    x_sum[...] = jnp.broadcast_to(jnp.sum(v * v, axis=1, keepdims=True), (2 * ROWS, 128))
    spliced = jnp.transpose(jnp.broadcast_to(mask_ref[...].astype(F32), (SEQ, SEQ)))
    level = level_ref[0].astype(F32)
    early_ref[...] = spliced * (1.0 - level)
    late_ref[...] = spliced * level
    cbuf[me] = clean_ref[...]
    for c in loads[2:6]:
        c.wait()
    pl.semaphore_wait(barrier, len(peers) + swaps.astype(jnp.int32))

    started = []

    def begin(c):
        c.start()
        started.append(c)

    def x_copy(k, target, to):
        return pltpu.make_async_remote_copy(
            src_ref=x_sum, dst_ref=x_got.at[to], send_sem=x_send.at[k], recv_sem=x_recv.at[to],
            device_id={"tp": target}, device_id_type=MESH,
        )

    def v_copy(h, k, x, z, where):
        return pltpu.make_async_remote_copy(
            src_ref=nsend.at[h], dst_ref=ngot.at[x, z], send_sem=v_send.at[h, k], recv_sem=v_recv.at[x, z],
            device_id=where, device_id_type=MESH,
        )

    def p_copy(k, source, to):
        return pltpu.make_async_remote_copy(
            src_ref=pbuf.at[source], dst_ref=pgot.at[to], send_sem=p_send.at[k], recv_sem=p_recv.at[to],
            device_id={"patch": w.block(0, k)}, device_id_type=MESH,
        )

    def w_copy(slot, dx, c, target):
        index = 2 * ((px + dx + 4) % 4) + c
        return pltpu.make_async_remote_copy(
            src_ref=wbuf.at[index], dst_ref=wbuf.at[index], send_sem=w_send.at[slot], recv_sem=w_recv.at[index],
            device_id={"patch": target}, device_id_type=MESH,
        )

    def s_copy(src, dst, send, recv, where):
        return pltpu.make_async_remote_copy(
            src_ref=src, dst_ref=dst, send_sem=s_send.at[send], recv_sem=recv,
            device_id=where, device_id_type=MESH,
        )

    for k, target in enumerate(others):
        begin(x_copy(k, target, t))
    begin(w_copy(0, 0, pc, w.block(1, 0)))
    begin(w_copy(1, 0, pc, w.block(3, 0)))
    begin(w_copy(2, 0, pc, partner))
    swap = s_copy(wo_ref, wo_own, 21, s_recv.at[10], {"patch": swap_p, "tp": swap_t})

    @pl.when(swaps)
    def _():
        swap.start()

    loads[6].wait()
    rows_dev = unembed_ref.shape[0]
    wanted = jnp.transpose(jnp.broadcast_to(ids_ref[...].astype(F32), (SCORED, SCORED)))[:, :1]
    wanted = wanted.astype(jnp.int32) - (me * NT + t) * rows_dev
    owned = jnp.where(
        wanted == lax.broadcasted_iota(jnp.int32, (SCORED, rows_dev), 1), 1.0, 0.0
    ).astype(BF16)
    for k in range(NT):
        chosen[k] = jnp.dot(
            owned, unembed_ref[:, FB * k : FB * (k + 1)], preferred_element_type=F32
        ).astype(BF16)
    half = SCORED // 2
    pair = s_copy(
        chosen.at[:, pl.ds(pl.multiple_of(half * (1 - pc), half), half)],
        chosen_got, 0, s_recv.at[0], {"patch": partner},
    )
    begin(pair)

    total = x_sum[...]
    for target in others:
        x_copy(0, target, target).wait_recv()
        total = total + x_got[target]
    scale = lax.rsqrt(total[:, :1] / D + EPSILON)
    v = (x_own[...] * scale * ngain_ref[...].astype(F32).reshape(1, FB)).astype(BF16)
    halves = []
    for h in range(2):
        nsend[h] = v[:, 256 * h : 256 * (h + 1)]
    for h in range(2):
        z_to = 2 * tz + h
        for k in range(NT):
            c = v_copy(h, k, ty, pz, {"patch": 8 * px + 2 * z_to + pc, "tp": (t + k) % NT})
            if k > 0:
                begin(c)
            else:
                halves.append((z_to, c))

                @pl.when(z_to != pz)
                def _(c=c):
                    c.start()

    @pl.when(pz // 2 == tz)
    def _():
        ngot[ty, pz] = nsend[pz % 2]

    w_copy(0, -w.way, pc, partner).wait_recv()
    begin(w_copy(3, -w.way, pc, w.block(w.way, 0)))
    begin(w_copy(4, -w.way, pc, partner))
    w_copy(0, w.way, pc, partner).wait_recv()
    begin(w_copy(5, w.way, pc, partner))

    @pl.when(swaps)
    def _():
        swap.wait_recv()

    @pl.when(jnp.logical_not(swaps))
    def _():
        wo_own[...] = wo_ref[...]

    o.z_send()
    pair.wait_recv()
    paired[...] = (
        chosen[:, pl.ds(pl.multiple_of(half * pc, half), half)] + chosen_got[...]
    ).reshape(4, 2, half, FB)
    y_others = [(k, (ty + k) % 4) for k in (1, 3, 2)]
    for k, y in y_others:
        begin(s_copy(paired.at[y], spread.at[ty], k, s_recv.at[1 + ty], {"tp": 2 * y + tz}))

    w_copy(0, 2, pc, partner).wait_recv()
    begin(w_copy(6, 2, pc, partner))
    for kz in range(4):
        z_from = (pz + kz) % 4
        for x in range(4):
            t_from = 2 * x + pz // 2
            c = v_copy(0, 0, x, z_from, {"patch": partner})
            if kz > 0:
                c.wait_recv()
            else:

                @pl.when(t_from != t)
                def _(c=c):
                    c.wait_recv()

    for dx in range(4):
        w_copy(0, dx, 1 - pc, partner).wait_recv()
    for x in range(4):
        piece = jnp.dot(
            ngot[x].reshape(8 * ROWS, 256), wbuf[2 * x : 2 * x + 2].reshape(256, WCOLS),
            preferred_element_type=F32,
        )
        if x == 0:
            acc[...] = piece
        else:
            acc[...] += piece
    pbuf[...] = acc[...].astype(BF16).reshape(4, 2 * ROWS, WCOLS)
    for k, target in z_others:
        begin(p_copy(k, target, pz))
    o.z_relay()
    o.own_send()
    obuf[me] = wo_own[...]

    v = paired[ty]
    for k, y in y_others:
        s_copy(paired.at[y], spread.at[y], 0, s_recv.at[1 + y], {"tp": 2 * y + tz}).wait_recv()
        v = v + spread[y]
    mine[...] = v
    begin(s_copy(mine.at[1 - tz], mine_got, 4, s_recv.at[5], {"tp": beside}))

    full = acc[pl.ds(pl.multiple_of(2 * ROWS * pz, 2 * ROWS), 2 * ROWS), :]
    for k, target in z_others:
        p_copy(k, target, target).wait_recv()
        full = full + pgot[target].astype(F32)

    at = pl.ds(pl.multiple_of((me * ROWS) % SEQ, ROWS), ROWS)
    cosine = jnp.concatenate([cos_ref[at, :]] * 2, axis=0)
    sine = jnp.concatenate([sin_ref[at, :]] * 2, axis=0)
    for h in range(WCOLS // HD):
        v = full[:, HD * h : HD * (h + 1)]
        if h < 5:
            v = v * cosine + pltpu.roll(v, HD // 2, 1) * sine
        v = v.astype(BF16)
        for s in range(2):
            qown[s, :, HD * h : HD * (h + 1)] = v[ROWS * s : ROWS * (s + 1)]
    qbuf[me] = qown[...]
    q.z_send()
    q.own_send()
    cl.z_send()
    o.z_forward(True)

    early = early_ref[...] > 0.5
    row = lax.broadcasted_iota(jnp.int32, (4 * SEQ, SEQ), 0) % SEQ
    col = lax.broadcasted_iota(jnp.int32, (4 * SEQ, SEQ), 1)
    causal = row >= col

    def a_copy(index, n, source, target):
        rows = pl.ds(SEQ * n, SEQ)
        return pltpu.make_async_remote_copy(
            src_ref=att.at[source, rows], dst_ref=att.at[source, rows],
            send_sem=a_send.at[index], recv_sem=a_recv.at[source, n],
            device_id={"tp": target}, device_id_type=MESH,
        )

    a_count = []

    def a_start(n, source, target):
        begin(a_copy(len(a_count), n, source, target))
        a_count.append(n)

    def a_wait(n, source):
        a_copy(0, n, source, others[0]).wait_recv()

    up, down, far_y = ((ty + 1) % 4) * 2, ((ty + 3) % 4) * 2, ((ty + 2) % 4) * 2
    near = (down, up)

    def across(n):
        return n < 2

    def clockwise(n):
        return n % 2 == 0

    def first(n):
        for y in near:
            a_wait(n, y + tz)
            if clockwise(n) == (y is down):
                a_start(n, y + tz, (up if y is down else down) + tz)
            if across(n):
                a_start(n, y + tz, beside)
        a_wait(n, beside)
        if not across(n):
            a_start(n, beside, up + tz)
            a_start(n, beside, down + tz)

    def second(n):
        a_wait(n, far_y + tz)
        if across(n):
            a_start(n, far_y + tz, beside)

    def crossed(n):
        for y in near:
            a_wait(n, y + 1 - tz)
            if not across(n) and clockwise(n) == (y is down):
                a_start(n, y + 1 - tz, (up if y is down else down) + tz)

    def third(n):
        a_wait(n, far_y + 1 - tz)

    prompts = [(px + dx) % 4 for dx in (0, 3, 1, 2)]

    def attend(n):
        prompt = prompts[n]

        def picked(lo, hi):
            a = qbuf[pl.ds(8 * prompt, 8), 0, :, lo:hi].reshape(SEQ, hi - lo).astype(F32)
            b = qbuf[pl.ds(8 * prompt, 8), 1, :, lo:hi].reshape(SEQ, hi - lo).astype(F32)
            return jnp.where(early, b, a).astype(BF16)

        queries = jnp.concatenate([picked(HD * h, HD * (h + 1)) for h in range(4)], axis=0)
        keys = picked(QCOLS, QCOLS + HD)
        values = picked(QCOLS + HD, QCOLS + 2 * HD)
        scores = lax.dot_general(
            queries, keys, (((1,), (1,)), ((), ())), preferred_element_type=F32
        ) * HD ** (-0.5)
        scores = jnp.where(causal, scores, -1e30)
        scores = jnp.exp(scores - jnp.max(scores, axis=1, keepdims=True))
        probs = (scores / jnp.sum(scores, axis=1, keepdims=True)).astype(BF16)
        heads = jnp.dot(probs, values, preferred_element_type=F32).astype(BF16)
        for h in range(4):
            att[t, SEQ * n : SEQ * (n + 1), HD * h : HD * (h + 1)] = heads[SEQ * h : SEQ * (h + 1)]
        for target in (up + tz, down + tz, beside):
            a_start(n, t, target)

    q.z_forward()
    q.x_near(0)
    q.core_wait(steps=(0,))
    attend(0)

    s_copy(mine.at[1 - tz], mine_got, 4, s_recv.at[5], {"tp": beside}).wait_recv()
    spread_z[...] = (mine[tz] + mine_got[...]).reshape(4, half // 4, FB)
    for k, target in z_others:
        begin(s_copy(spread_z.at[target], sum_z.at[pz], 8 + k, sz_recv.at[pz], {"patch": w.block(0, k)}))

    cl.z_relay()
    q.x_forward()
    o.x_near(0)
    q.core_wait(steps=(3, 1))
    attend(1)
    attend(2)

    v = spread_z[pz]
    for k, target in z_others:
        s_copy(spread_z.at[target], sum_z.at[target], 0, sz_recv.at[target], {"patch": w.block(0, k)}).wait_recv()
        v = v + sum_z[target]
    own_x[...] = v
    for k, target in x_others:
        begin(s_copy(own_x, sum_x.at[px], 12 + k, sx_recv.at[px], {"patch": w.block(k, 0)}))

    first(0)
    cl.own_send()
    cl.z_forward(True)
    q.far()
    q.core_wait(steps=(2,))
    attend(3)
    o.x_near(1)

    v = own_x[...]
    for k, target in x_others:
        s_copy(own_x, sum_x.at[target], 0, sx_recv.at[target], {"patch": w.block(k, 0)}).wait_recv()
        v = v + sum_x[target]
    score[pc, pz] = v
    for k, target in z_others:
        begin(s_copy(score.at[pc, pz], score.at[pc, pz], 16 + k, sg_recv.at[pz], {"patch": w.block(0, k)}))

    last = far_y + 1 - tz

    def project(n, count, sources, fresh=False):
        rows = pl.ds(SEQ * n, SEQ * count)
        for k, source in enumerate(sources):
            block = jnp.concatenate([obuf[4 * source + j] for j in range(4)], axis=1)
            piece = jnp.dot(att[source, rows], block, preferred_element_type=F32)
            if fresh and k == 0:
                head[rows] = piece
            else:
                head[rows] += piece

    first(1)
    first(2)
    second(0)

    o.x_near(2)
    o.x_near(3)
    first(3)
    for k, target in z_others:
        s_copy(score.at[pc, target], score.at[pc, target], 0, sg_recv.at[target], {"patch": w.block(0, k)}).wait_recv()
    begin(s_copy(score.at[pc], score.at[pc], 20, s_recv.at[9], {"patch": partner}))
    second(1)
    crossed(2)
    cl.x_forward(first=0)

    o.far()
    crossed(3)
    o.core_wait()
    project(0, 4, (t, beside, up + tz, down + tz), True)
    cl.far()
    crossed(0)
    crossed(1)
    second(2)
    second(3)
    project(0, 4, (far_y + tz, up + 1 - tz, down + 1 - tz))
    s_copy(score.at[pc], score.at[1 - pc], 0, s_recv.at[9], {"patch": partner}).wait_recv()
    score_t[...] = jnp.transpose(score[...].reshape(SCORED, FB).astype(F32)).astype(BF16)
    cl.core_wait()

    gain = fgain_ref[...].astype(F32).reshape(1, FB)
    share = TOKENS // NT

    def l_copy(target, to):
        return pltpu.make_async_remote_copy(
            src_ref=lg.at[target], dst_ref=lg_got.at[to], send_sem=l_send.at[target], recv_sem=l_recv.at[to],
            device_id={"tp": target}, device_id_type=MESH,
        )

    def n_copy(target, to):
        return pltpu.make_async_remote_copy(
            src_ref=ssq.at[target // 2], dst_ref=ssq_got.at[to], send_sem=n_send.at[target], recv_sem=n_recv.at[to],
            device_id={"tp": target}, device_id_type=MESH,
        )

    for n in range(PROMPTS):
        if n == 0:
            third(0)
            third(1)
            project(0, 2, (last,))
        if n == 2:
            third(2)
            third(3)
            project(2, 2, (last,))

        def finish(i, carry, n=n):
            at = pl.ds(pl.multiple_of(SEQ * n + ROWS * i, ROWS), ROWS)
            token = pl.ds(pl.multiple_of(SEQ * prompts[n] + ROWS * i, ROWS), ROWS)
            local_at = pl.ds(pl.multiple_of(ROWS * i, ROWS), ROWS)
            e = early_ref[local_at, :1] > 0.5
            late = late_ref[local_at, :1] > 0.5
            v = corrupt_ref[token, :].astype(F32)
            v = jnp.where(e, cbuf[8 * prompts[n] + i, 0].astype(F32), v)
            v = v + head[at, :]
            v = jnp.where(late, cbuf[8 * prompts[n] + i, 1].astype(F32), v)
            squares[local_at, :] = jnp.broadcast_to(
                jnp.sum(v * v, axis=1, keepdims=True), (ROWS, 128)
            )
            fin[local_at, :] = (v * gain).astype(BF16)
            return carry

        lax.fori_loop(0, SEQ // ROWS, finish, 0, unroll=4)
        ssq[prompts[n]] = jnp.transpose(squares[...])[:8]
        value = jnp.dot(fin[...], score_t[...], preferred_element_type=F32).astype(BF16)
        for s in range(2):
            target = 2 * prompts[n] + s
            lg[target] = value[share * s : share * (s + 1)]

            @pl.when(target != t)
            def _(target=target):
                n_copy(target, t).start()
                l_copy(target, t).start()

    logits = lg[t].astype(F32)
    total = ssq[ty]
    for target in others:
        n_copy(target, target).wait_recv()
        l_copy(target, target).wait_recv()
        logits = logits + lg_got[target].astype(F32)
        total = total + ssq_got[target]
    scale = jnp.transpose(jnp.broadcast_to(lax.rsqrt(total[:1] / D + EPSILON), (SEQ, SEQ)))
    scale = jnp.where(tz == 0, scale[:share], scale[share:])
    out_ref[...] = logits * scale[:, :1]

    for target in others:
        n_copy(target, t).wait_send()
        l_copy(target, t).wait_send()

    @pl.when(swaps)
    def _():
        swap.wait_send()

    for z_to, c in halves:

        @pl.when(z_to != pz)
        def _(c=c):
            c.wait_send()

    for c in started:
        c.wait_send()
    for g in (q, o, cl):
        g.drain()


def layer(*operands):
    vmem = pl.BlockSpec(memory_space=pltpu.VMEM)
    smem = pl.BlockSpec(memory_space=pltpu.SMEM)
    hbm = pl.BlockSpec(memory_space=pl.ANY)
    dma = pltpu.SemaphoreType.DMA
    share = TOKENS // NT
    half = SCORED // 2
    rows_dev = operands[6].shape[0]
    return pl.pallas_call(
        layer_kernel,
        out_shape=jax.ShapeDtypeStruct((share, SCORED), F32),
        in_specs=[hbm] * 7 + [smem] + [vmem] * 6,
        out_specs=vmem,
        scratch_shapes=[
            pltpu.VMEM((TOKENS, FB), BF16),
            pltpu.VMEM((2, ROWS, FB), BF16),
            pltpu.VMEM((FB, 128), BF16),
            pltpu.VMEM((FB, 128), BF16),
            pltpu.VMEM((rows_dev, D), BF16),
            pltpu.VMEM((2 * ROWS, FB), F32),
            pltpu.VMEM((2 * ROWS, 128), F32),
            pltpu.VMEM((NT, 2 * ROWS, 128), F32),
            pltpu.VMEM((2, 2 * ROWS, 256), BF16),
            pltpu.VMEM((4, 4, 2 * ROWS, 256), BF16),
            pltpu.VMEM((8, 128, WCOLS), BF16),
            pltpu.VMEM((8 * ROWS, WCOLS), F32),
            pltpu.VMEM((4, 2 * ROWS, WCOLS), BF16),
            pltpu.VMEM((4, 2 * ROWS, WCOLS), BF16),
            pltpu.VMEM((2, ROWS, WCOLS), BF16),
            pltpu.VMEM((NP, 2, ROWS, WCOLS), BF16),
            pltpu.VMEM((NP, FB, 128), BF16),
            pltpu.VMEM((NP, 2, ROWS, FB), BF16),
            pltpu.VMEM((NT, TOKENS, FB), BF16),
            pltpu.VMEM((TOKENS, FB), F32),
            pltpu.VMEM((SEQ, SEQ), F32),
            pltpu.VMEM((SEQ, SEQ), F32),
            pltpu.VMEM((NT, SCORED, FB), BF16),
            pltpu.VMEM((NT, half, FB), BF16),
            pltpu.VMEM((4, 2, half, FB), BF16),
            pltpu.VMEM((4, 2, half, FB), BF16),
            pltpu.VMEM((2, half, FB), BF16),
            pltpu.VMEM((half, FB), BF16),
            pltpu.VMEM((4, half // 4, FB), BF16),
            pltpu.VMEM((4, half // 4, FB), BF16),
            pltpu.VMEM((4, half // 4, FB), BF16),
            pltpu.VMEM((half // 4, FB), BF16),
            pltpu.VMEM((2, 4, half // 4, FB), BF16),
            pltpu.VMEM((SEQ, FB), BF16),
            pltpu.VMEM((FB, SCORED), BF16),
            pltpu.VMEM((SEQ, 128), F32),
            pltpu.VMEM((PROMPTS, 8, 128), F32),
            pltpu.VMEM((NT, 8, 128), F32),
            pltpu.VMEM((NT, share, SCORED), BF16),
            pltpu.VMEM((NT, share, SCORED), BF16),
            dma((7,)),
            dma((NT,)), dma((NT,)),
            dma((2, NT)), dma((4, 4)),
            dma((4,)), dma((4,)),
            dma((7,)), dma((8,)),
            dma((N_SENDS,)), dma((NP,)),
            dma((N_SENDS,)), dma((NP,)),
            dma((N_SENDS,)), dma((NP,)),
            dma((32,)), dma((NT, PROMPTS)),
            dma((22,)), dma((11,)), dma((4,)), dma((4,)), dma((4,)),
            dma((NT,)), dma((NT,)), dma((NT,)), dma((NT,)),
        ],
        compiler_params=pltpu.CompilerParams(
            collective_id=0, has_side_effects=True, vmem_limit_bytes=60 * 1024 * 1024
        ),
        cost_estimate=pl.CostEstimate(
            flops=4 * 10**9, bytes_accessed=20 * 2**20, transcendentals=10**6
        ),
        name="layer",
    )(*operands)


def rope_tables():
    half = HD // 2
    exponents = -(np.arange(half, dtype=np.float32) * np.float32(2.0 / HD))
    freqs = (np.float32(THETA) ** exponents).astype(np.float32)
    angles = np.arange(SEQ, dtype=np.float32)[:, None] * freqs[None, :]
    cosine, sine = np.cos(angles), np.sin(angles)
    return (
        np.concatenate([cosine, cosine], axis=1).astype(np.float32),
        np.concatenate([-sine, sine], axis=1).astype(np.float32),
    )


def on_device(
    resid_corrupt, resid_clean, patch_level, patch_mask, norm_gain, final_gain,
    w_query, w_key, w_value, w_out, unembed, scored_ids, base_logits,
):
    cosine, sine = rope_tables()
    out = layer(
        resid_corrupt, resid_clean, w_query, w_key, w_value, w_out, unembed,
        patch_level, patch_mask, scored_ids[None, :], norm_gain, final_gain, jnp.asarray(cosine), jnp.asarray(sine),
    )
    return (out - base_logits)[None]


def solution(mesh):
    placed = (
        P(None, "tp"),
        P(None, "patch", "tp"),
        P("patch"),
        P("patch", None),
        P("tp"),
        P("tp"),
        P("patch", "tp"),
        P("patch", "tp"),
        P("patch", "tp"),
        P("tp", "patch"),
        P(("patch", "tp"), None),
        P(),
        P("tp", None),
    )
    return jax.shard_map(
        on_device, mesh=mesh, in_specs=placed, out_specs=P("patch", "tp", None), check_vma=False
    )
```

```python
import jax
import jax.numpy as jnp
import numpy as np
from jax import lax
from jax.experimental import pallas as pl
from jax.experimental.pallas import tpu as pltpu
from jax.sharding import PartitionSpec as P

D = 4096
HD = 128
SEQ = 128
PROMPTS = 4
TOKENS = PROMPTS * SEQ
SCORED = 256
NP = 32
NT = 8
FB = D // NT
ROWS = TOKENS // NP
QCOLS = 512
KVCOL = 128
WCOLS = QCOLS + 2 * KVCOL
EPSILON = 1e-05
THETA = 500000.0
MESH = pl.DeviceIdType.MESH
F32 = jnp.float32
BF16 = jnp.bfloat16
N_SENDS = 31


class PatchGather:
    def __init__(self, own, buf, send, recv):
        self.own, self.buf, self.send, self.recv = own, buf, send, recv
        me = lax.axis_index("patch")
        self.me = me
        self.x, self.z, self.c = me // 8, (me // 2) % 4, me % 2
        self.way = 1 - 2 * self.c
        self.started = []

    def block(self, dx, dz, other=False):
        c = 1 - self.c if other else self.c
        return ((self.x + dx) % 4) * 8 + ((self.z + dz + 4) % 4) * 2 + c

    def copy(self, src, index, target, slot):
        return pltpu.make_async_remote_copy(
            src_ref=src,
            dst_ref=self.buf.at[index],
            send_sem=self.send.at[slot],
            recv_sem=self.recv.at[index],
            device_id={"patch": target},
            device_id_type=MESH,
        )

    def start(self, src, index, target):
        c = self.copy(src, index, target, len(self.started))
        c.start()
        self.started.append(c)

    def wait(self, index):
        self.copy(self.buf.at[index], index, self.block(1, 0), 0).wait_recv()

    def z_send(self):
        for dz in (self.way, -self.way):
            self.start(self.own, self.me, self.block(0, dz))

    def own_send(self):
        for target in (self.block(1, 0), self.block(3, 0), self.block(0, 0, True)):
            self.start(self.own, self.me, target)

    def z_relay(self):
        b = self.block(0, -self.way)
        self.wait(b)
        self.start(self.buf.at[b], b, self.block(0, self.way))

    def spread(self, b):
        for target in (self.block(1, 0), self.block(3, 0), self.block(0, 0, True)):
            self.start(self.buf.at[b], b, target)

    def z_forward(self, relayed=False):
        if not relayed:
            self.z_relay()
        for k, dz in enumerate((-self.way, self.way, 2)):
            b = self.block(0, dz)
            if k > 0:
                self.wait(b)
            self.spread(b)

    def x_near(self, k, then=None):
        for dx in (3, 1):
            b = self.block(dx, (0, -self.way, self.way, 2)[k])
            self.wait(b)
            if (k in (0, 3)) == (dx == 3):
                self.start(self.buf.at[b], b, self.block(4 - dx, 0))
            self.start(self.buf.at[b], b, self.block(0, 0, True))
            if then is not None:
                then(b)

    def x_forward(self, then=None, first=1):
        for k in range(first, 4):
            self.x_near(k, then)

    def far(self, then=None):
        for dz in (0, -self.way, self.way, 2):
            b = self.block(2, dz)
            self.wait(b)
            self.start(self.buf.at[b], b, self.block(0, 0, True))
            if then is not None:
                then(b)

    def core_wait(self, then=None, steps=(0, 3, 1, 2)):
        for dx in steps:
            for dz in (0, self.way, -self.way, 2):
                b = self.block(dx, dz, True)
                self.wait(b)
                if then is not None:
                    then(b)

    def drain(self):
        for c in self.started:
            c.wait_send()


def layer_kernel(
    corrupt_hbm, clean_hbm, wq_hbm, wk_hbm, wv_hbm, wo_hbm, unembed_hbm,
    level_ref, mask_ref, ids_ref, ngain_ref, fgain_ref, cos_ref, sin_ref,
    out_ref,
    corrupt_ref, clean_ref, wo_ref, wo_own, unembed_ref,
    x_own, x_sum, x_got, nsend, ngot, wbuf, acc, pbuf, pgot, qown, qbuf, obuf, cbuf, att, head, early_ref, late_ref,
    chosen, chosen_got, paired, spread, mine, mine_got, spread_z, sum_z, sum_x, own_x, score, fin, score_t, squares, ssq, ssq_got, lg, lg_got,
    local, x_send, x_recv, v_send, v_recv, p_send, p_recv, w_send, w_recv, q_send, q_recv, o_send, o_recv, c_send, c_recv, a_send, a_recv,
    s_send, s_recv, sz_recv, sx_recv, sg_recv, l_send, l_recv, n_send, n_recv,
):
    t = lax.axis_index("tp")
    q = PatchGather(qown, qbuf, q_send, q_recv)
    o = PatchGather(wo_own, obuf, o_send, o_recv)
    cl = PatchGather(clean_ref, cbuf, c_send, c_recv)
    w = q
    me, px, pz, pc = w.me, w.x, w.z, w.c
    ty, tz = t // 2, t % 2
    beside = t + 1 - 2 * tz
    others = [(t + k) % NT for k in range(1, NT)]
    z_others = [(k, (pz + k) % 4) for k in (1, 3, 2)]
    x_others = [(k, (px + k) % 4) for k in (1, 3, 2)]
    partner = w.block(0, 0, True)
    swap_p, swap_t = 4 * t + me % 4, me // 4
    swaps = swap_t != t

    loads = [
        pltpu.make_async_copy(src, dst, local.at[k])
        for k, (src, dst) in enumerate(
            [
                (corrupt_hbm, corrupt_ref),
                (clean_hbm, clean_ref),
                (wq_hbm, wbuf.at[2 * px + pc, :, pl.ds(0, QCOLS)]),
                (wk_hbm, wbuf.at[2 * px + pc, :, pl.ds(QCOLS, KVCOL)]),
                (wv_hbm, wbuf.at[2 * px + pc, :, pl.ds(QCOLS + KVCOL, KVCOL)]),
                (wo_hbm, wo_ref),
                (unembed_hbm, unembed_ref),
            ]
        )
    ]
    for c in loads:
        c.start()
    barrier = pltpu.get_barrier_semaphore()
    peers = (
        [{"tp": k} for k in others]
        + [{"patch": w.block(0, dz)} for dz in (1, 3, 2)]
        + [{"patch": w.block(dx, 0)} for dx in (1, 3, 2)]
        + [{"patch": partner}]
        + [{"patch": w.block(0, dz), "tp": k} for dz in (1, 3, 2) for k in others]
    )
    for peer in peers:
        pl.semaphore_signal(barrier, inc=1, device_id=peer, device_id_type=MESH)

    @pl.when(swaps)
    def _():
        pl.semaphore_signal(
            barrier, inc=1, device_id={"patch": swap_p, "tp": swap_t}, device_id_type=MESH
        )

    for c in loads[:2]:
        c.wait()
    x_own[:ROWS] = corrupt_ref[pl.ds(pl.multiple_of(me * ROWS, ROWS), ROWS), :].astype(F32)
    x_own[ROWS:] = clean_ref[0].astype(F32)
    v = x_own[...]
    x_sum[...] = jnp.broadcast_to(jnp.sum(v * v, axis=1, keepdims=True), (2 * ROWS, 128))
    spliced = jnp.transpose(jnp.broadcast_to(mask_ref[...].astype(F32), (SEQ, SEQ)))
    level = level_ref[0].astype(F32)
    early_ref[...] = spliced * (1.0 - level)
    late_ref[...] = spliced * level
    cbuf[me] = clean_ref[...]
    for c in loads[2:6]:
        c.wait()
    pl.semaphore_wait(barrier, len(peers) + swaps.astype(jnp.int32))

    started = []

    def begin(c):
        c.start()
        started.append(c)

    def x_copy(k, target, to):
        return pltpu.make_async_remote_copy(
            src_ref=x_sum, dst_ref=x_got.at[to], send_sem=x_send.at[k], recv_sem=x_recv.at[to],
            device_id={"tp": target}, device_id_type=MESH,
        )

    def v_copy(h, k, x, z, where):
        return pltpu.make_async_remote_copy(
            src_ref=nsend.at[h], dst_ref=ngot.at[x, z], send_sem=v_send.at[h, k], recv_sem=v_recv.at[x, z],
            device_id=where, device_id_type=MESH,
        )

    def p_copy(k, source, to):
        return pltpu.make_async_remote_copy(
            src_ref=pbuf.at[source], dst_ref=pgot.at[to], send_sem=p_send.at[k], recv_sem=p_recv.at[to],
            device_id={"patch": w.block(0, k)}, device_id_type=MESH,
        )

    def w_copy(slot, dx, c, target):
        index = 2 * ((px + dx + 4) % 4) + c
        return pltpu.make_async_remote_copy(
            src_ref=wbuf.at[index], dst_ref=wbuf.at[index], send_sem=w_send.at[slot], recv_sem=w_recv.at[index],
            device_id={"patch": target}, device_id_type=MESH,
        )

    def s_copy(src, dst, send, recv, where):
        return pltpu.make_async_remote_copy(
            src_ref=src, dst_ref=dst, send_sem=s_send.at[send], recv_sem=recv,
            device_id=where, device_id_type=MESH,
        )

    for k, target in enumerate(others):
        begin(x_copy(k, target, t))
    begin(w_copy(0, 0, pc, w.block(1, 0)))
    begin(w_copy(1, 0, pc, w.block(3, 0)))
    begin(w_copy(2, 0, pc, partner))
    swap = s_copy(wo_ref, wo_own, 21, s_recv.at[10], {"patch": swap_p, "tp": swap_t})

    @pl.when(swaps)
    def _():
        swap.start()

    loads[6].wait()
    rows_dev = unembed_ref.shape[0]
    wanted = jnp.transpose(jnp.broadcast_to(ids_ref[...].astype(F32), (SCORED, SCORED)))[:, :1]
    wanted = wanted.astype(jnp.int32) - (me * NT + t) * rows_dev
    owned = jnp.where(
        wanted == lax.broadcasted_iota(jnp.int32, (SCORED, rows_dev), 1), 1.0, 0.0
    ).astype(BF16)
    for k in range(NT):
        chosen[k] = jnp.dot(
            owned, unembed_ref[:, FB * k : FB * (k + 1)], preferred_element_type=F32
        ).astype(BF16)
    half = SCORED // 2
    pair = s_copy(
        chosen.at[:, pl.ds(pl.multiple_of(half * (1 - pc), half), half)],
        chosen_got, 0, s_recv.at[0], {"patch": partner},
    )
    begin(pair)

    total = x_sum[...]
    for target in others:
        x_copy(0, target, target).wait_recv()
        total = total + x_got[target]
    scale = lax.rsqrt(total[:, :1] / D + EPSILON)
    v = (x_own[...] * scale * ngain_ref[...].astype(F32).reshape(1, FB)).astype(BF16)
    halves = []
    for h in range(2):
        nsend[h] = v[:, 256 * h : 256 * (h + 1)]
    for h in range(2):
        z_to = 2 * tz + h
        for k in range(NT):
            c = v_copy(h, k, ty, pz, {"patch": 8 * px + 2 * z_to + pc, "tp": (t + k) % NT})
            if k > 0:
                begin(c)
            else:
                halves.append((z_to, c))

                @pl.when(z_to != pz)
                def _(c=c):
                    c.start()

    @pl.when(pz // 2 == tz)
    def _():
        ngot[ty, pz] = nsend[pz % 2]

    w_copy(0, -w.way, pc, partner).wait_recv()
    begin(w_copy(3, -w.way, pc, w.block(w.way, 0)))
    begin(w_copy(4, -w.way, pc, partner))
    w_copy(0, w.way, pc, partner).wait_recv()
    begin(w_copy(5, w.way, pc, partner))

    @pl.when(swaps)
    def _():
        swap.wait_recv()

    @pl.when(jnp.logical_not(swaps))
    def _():
        wo_own[...] = wo_ref[...]

    o.z_send()
    pair.wait_recv()
    paired[...] = (
        chosen[:, pl.ds(pl.multiple_of(half * pc, half), half)] + chosen_got[...]
    ).reshape(4, 2, half, FB)
    y_others = [(k, (ty + k) % 4) for k in (1, 3, 2)]
    for k, y in y_others:
        begin(s_copy(paired.at[y], spread.at[ty], k, s_recv.at[1 + ty], {"tp": 2 * y + tz}))

    w_copy(0, 2, pc, partner).wait_recv()
    begin(w_copy(6, 2, pc, partner))
    for kz in range(4):
        z_from = (pz + kz) % 4
        for x in range(4):
            t_from = 2 * x + pz // 2
            c = v_copy(0, 0, x, z_from, {"patch": partner})
            if kz > 0:
                c.wait_recv()
            else:

                @pl.when(t_from != t)
                def _(c=c):
                    c.wait_recv()

    for dx in range(4):
        w_copy(0, dx, 1 - pc, partner).wait_recv()
    for x in range(4):
        piece = jnp.dot(
            ngot[x].reshape(8 * ROWS, 256), wbuf[2 * x : 2 * x + 2].reshape(256, WCOLS),
            preferred_element_type=F32,
        )
        if x == 0:
            acc[...] = piece
        else:
            acc[...] += piece
    pbuf[...] = acc[...].astype(BF16).reshape(4, 2 * ROWS, WCOLS)
    for k, target in z_others:
        begin(p_copy(k, target, pz))
    o.z_relay()
    o.own_send()
    obuf[me] = wo_own[...]


    full = acc[pl.ds(pl.multiple_of(2 * ROWS * pz, 2 * ROWS), 2 * ROWS), :]
    for k, target in z_others:
        p_copy(k, target, target).wait_recv()
        full = full + pgot[target].astype(F32)

    at = pl.ds(pl.multiple_of((me * ROWS) % SEQ, ROWS), ROWS)
    cosine = jnp.concatenate([cos_ref[at, :]] * 2, axis=0)
    sine = jnp.concatenate([sin_ref[at, :]] * 2, axis=0)
    for h in range(WCOLS // HD):
        v = full[:, HD * h : HD * (h + 1)]
        if h < 5:
            v = v * cosine + pltpu.roll(v, HD // 2, 1) * sine
        v = v.astype(BF16)
        for s in range(2):
            qown[s, :, HD * h : HD * (h + 1)] = v[ROWS * s : ROWS * (s + 1)]
    qbuf[me] = qown[...]
    q.z_send()
    q.own_send()
    cl.z_send()
    v = paired[ty]
    for k, y in y_others:
        s_copy(paired.at[y], spread.at[y], 0, s_recv.at[1 + y], {"tp": 2 * y + tz}).wait_recv()
        v = v + spread[y]
    mine[...] = v
    begin(s_copy(mine.at[1 - tz], mine_got, 4, s_recv.at[5], {"tp": beside}))
    o.z_forward(True)

    early = early_ref[...] > 0.5
    row = lax.broadcasted_iota(jnp.int32, (4 * SEQ, SEQ), 0) % SEQ
    col = lax.broadcasted_iota(jnp.int32, (4 * SEQ, SEQ), 1)
    causal = row >= col

    def a_copy(index, n, source, target):
        rows = pl.ds(SEQ * n, SEQ)
        return pltpu.make_async_remote_copy(
            src_ref=att.at[source, rows], dst_ref=att.at[source, rows],
            send_sem=a_send.at[index], recv_sem=a_recv.at[source, n],
            device_id={"tp": target}, device_id_type=MESH,
        )

    a_count = []

    def a_start(n, source, target):
        begin(a_copy(len(a_count), n, source, target))
        a_count.append(n)

    def a_wait(n, source):
        a_copy(0, n, source, others[0]).wait_recv()

    up, down, far_y = ((ty + 1) % 4) * 2, ((ty + 3) % 4) * 2, ((ty + 2) % 4) * 2
    near = (down, up)

    def across(n):
        return n < 2

    def clockwise(n):
        return n % 2 == 0

    def first(n):
        for y in near:
            a_wait(n, y + tz)
            if clockwise(n) == (y is down):
                a_start(n, y + tz, (up if y is down else down) + tz)
            if across(n):
                a_start(n, y + tz, beside)
        a_wait(n, beside)
        if not across(n):
            a_start(n, beside, up + tz)
            a_start(n, beside, down + tz)

    def second(n):
        a_wait(n, far_y + tz)
        if across(n):
            a_start(n, far_y + tz, beside)

    def crossed(n):
        for y in near:
            a_wait(n, y + 1 - tz)
            if not across(n) and clockwise(n) == (y is down):
                a_start(n, y + 1 - tz, (up if y is down else down) + tz)

    def third(n):
        a_wait(n, far_y + 1 - tz)

    prompts = [(px + dx) % 4 for dx in (0, 3, 1, 2)]

    def attend(n):
        prompt = prompts[n]

        def picked(lo, hi):
            a = qbuf[pl.ds(8 * prompt, 8), 0, :, lo:hi].reshape(SEQ, hi - lo).astype(F32)
            b = qbuf[pl.ds(8 * prompt, 8), 1, :, lo:hi].reshape(SEQ, hi - lo).astype(F32)
            return jnp.where(early, b, a).astype(BF16)

        queries = jnp.concatenate([picked(HD * h, HD * (h + 1)) for h in range(4)], axis=0)
        keys = picked(QCOLS, QCOLS + HD)
        values = picked(QCOLS + HD, QCOLS + 2 * HD)
        scores = lax.dot_general(
            queries, keys, (((1,), (1,)), ((), ())), preferred_element_type=F32
        ) * HD ** (-0.5)
        scores = jnp.where(causal, scores, -1e30)
        scores = jnp.exp(scores - jnp.max(scores, axis=1, keepdims=True))
        probs = (scores / jnp.sum(scores, axis=1, keepdims=True)).astype(BF16)
        heads = jnp.dot(probs, values, preferred_element_type=F32).astype(BF16)
        for h in range(4):
            att[t, SEQ * n : SEQ * (n + 1), HD * h : HD * (h + 1)] = heads[SEQ * h : SEQ * (h + 1)]
        for target in (up + tz, down + tz, beside):
            a_start(n, t, target)

    q.z_forward()
    q.x_near(0)
    q.core_wait(steps=(0,))
    attend(0)

    s_copy(mine.at[1 - tz], mine_got, 4, s_recv.at[5], {"tp": beside}).wait_recv()
    spread_z[...] = (mine[tz] + mine_got[...]).reshape(4, half // 4, FB)
    for k, target in z_others:
        begin(s_copy(spread_z.at[target], sum_z.at[pz], 8 + k, sz_recv.at[pz], {"patch": w.block(0, k)}))

    cl.z_relay()
    q.x_forward()
    o.x_near(0)
    q.core_wait(steps=(3, 1))
    attend(1)
    attend(2)

    v = spread_z[pz]
    for k, target in z_others:
        s_copy(spread_z.at[target], sum_z.at[target], 0, sz_recv.at[target], {"patch": w.block(0, k)}).wait_recv()
        v = v + sum_z[target]
    own_x[...] = v
    for k, target in x_others:
        begin(s_copy(own_x, sum_x.at[px], 12 + k, sx_recv.at[px], {"patch": w.block(k, 0)}))

    first(0)
    cl.own_send()
    cl.z_forward(True)
    q.far()
    q.core_wait(steps=(2,))
    attend(3)
    o.x_near(1)

    v = own_x[...]
    for k, target in x_others:
        s_copy(own_x, sum_x.at[target], 0, sx_recv.at[target], {"patch": w.block(k, 0)}).wait_recv()
        v = v + sum_x[target]
    score[pc, pz] = v
    for k, target in z_others:
        begin(s_copy(score.at[pc, pz], score.at[pc, pz], 16 + k, sg_recv.at[pz], {"patch": w.block(0, k)}))

    last = far_y + 1 - tz

    def project(n, count, sources, fresh=False):
        rows = pl.ds(SEQ * n, SEQ * count)
        for k, source in enumerate(sources):
            block = jnp.concatenate([obuf[4 * source + j] for j in range(4)], axis=1)
            piece = jnp.dot(att[source, rows], block, preferred_element_type=F32)
            if fresh and k == 0:
                head[rows] = piece
            else:
                head[rows] += piece

    first(1)
    first(2)
    second(0)

    o.x_near(2)
    o.x_near(3)
    first(3)
    second(1)
    crossed(2)
    cl.x_forward(first=0)

    o.far()
    crossed(3)
    for k, target in z_others:
        s_copy(score.at[pc, target], score.at[pc, target], 0, sg_recv.at[target], {"patch": w.block(0, k)}).wait_recv()
    begin(s_copy(score.at[pc], score.at[pc], 20, s_recv.at[9], {"patch": partner}))
    o.core_wait()
    project(0, 4, (t, beside, up + tz, down + tz), True)
    cl.far()
    crossed(0)
    crossed(1)
    second(2)
    second(3)
    project(0, 4, (far_y + tz, up + 1 - tz, down + 1 - tz))
    s_copy(score.at[pc], score.at[1 - pc], 0, s_recv.at[9], {"patch": partner}).wait_recv()
    score_t[...] = jnp.transpose(score[...].reshape(SCORED, FB).astype(F32)).astype(BF16)
    cl.core_wait()

    gain = fgain_ref[...].astype(F32).reshape(1, FB)
    share = TOKENS // NT

    def l_copy(target, to):
        return pltpu.make_async_remote_copy(
            src_ref=lg.at[target], dst_ref=lg_got.at[to], send_sem=l_send.at[target], recv_sem=l_recv.at[to],
            device_id={"tp": target}, device_id_type=MESH,
        )

    def n_copy(target, to):
        return pltpu.make_async_remote_copy(
            src_ref=ssq.at[target // 2], dst_ref=ssq_got.at[to], send_sem=n_send.at[target], recv_sem=n_recv.at[to],
            device_id={"tp": target}, device_id_type=MESH,
        )

    for n in range(PROMPTS):
        if n == 0:
            third(0)
            third(1)
            project(0, 2, (last,))
        if n == 2:
            third(2)
            third(3)
            project(2, 2, (last,))

        def finish(i, carry, n=n):
            at = pl.ds(pl.multiple_of(SEQ * n + ROWS * i, ROWS), ROWS)
            token = pl.ds(pl.multiple_of(SEQ * prompts[n] + ROWS * i, ROWS), ROWS)
            local_at = pl.ds(pl.multiple_of(ROWS * i, ROWS), ROWS)
            e = early_ref[local_at, :1] > 0.5
            late = late_ref[local_at, :1] > 0.5
            v = corrupt_ref[token, :].astype(F32)
            v = jnp.where(e, cbuf[8 * prompts[n] + i, 0].astype(F32), v)
            v = v + head[at, :]
            v = jnp.where(late, cbuf[8 * prompts[n] + i, 1].astype(F32), v)
            squares[local_at, :] = jnp.broadcast_to(
                jnp.sum(v * v, axis=1, keepdims=True), (ROWS, 128)
            )
            fin[local_at, :] = (v * gain).astype(BF16)
            return carry

        lax.fori_loop(0, SEQ // ROWS, finish, 0, unroll=4)
        ssq[prompts[n]] = jnp.transpose(squares[...])[:8]
        value = jnp.dot(fin[...], score_t[...], preferred_element_type=F32).astype(BF16)
        for s in range(2):
            target = 2 * prompts[n] + s
            lg[target] = value[share * s : share * (s + 1)]

            @pl.when(target != t)
            def _(target=target):
                n_copy(target, t).start()
                l_copy(target, t).start()

    logits = lg[t].astype(F32)
    total = ssq[ty]
    for target in others:
        n_copy(target, target).wait_recv()
        l_copy(target, target).wait_recv()
        logits = logits + lg_got[target].astype(F32)
        total = total + ssq_got[target]
    scale = jnp.transpose(jnp.broadcast_to(lax.rsqrt(total[:1] / D + EPSILON), (SEQ, SEQ)))
    scale = jnp.where(tz == 0, scale[:share], scale[share:])
    out_ref[...] = logits * scale[:, :1]

    for target in others:
        n_copy(target, t).wait_send()
        l_copy(target, t).wait_send()

    @pl.when(swaps)
    def _():
        swap.wait_send()

    for z_to, c in halves:

        @pl.when(z_to != pz)
        def _(c=c):
            c.wait_send()

    for c in started:
        c.wait_send()
    for g in (q, o, cl):
        g.drain()


def layer(*operands):
    vmem = pl.BlockSpec(memory_space=pltpu.VMEM)
    smem = pl.BlockSpec(memory_space=pltpu.SMEM)
    hbm = pl.BlockSpec(memory_space=pl.ANY)
    dma = pltpu.SemaphoreType.DMA
    share = TOKENS // NT
    half = SCORED // 2
    rows_dev = operands[6].shape[0]
    return pl.pallas_call(
        layer_kernel,
        out_shape=jax.ShapeDtypeStruct((share, SCORED), F32),
        in_specs=[hbm] * 7 + [smem] + [vmem] * 6,
        out_specs=vmem,
        scratch_shapes=[
            pltpu.VMEM((TOKENS, FB), BF16),
            pltpu.VMEM((2, ROWS, FB), BF16),
            pltpu.VMEM((FB, 128), BF16),
            pltpu.VMEM((FB, 128), BF16),
            pltpu.VMEM((rows_dev, D), BF16),
            pltpu.VMEM((2 * ROWS, FB), F32),
            pltpu.VMEM((2 * ROWS, 128), F32),
            pltpu.VMEM((NT, 2 * ROWS, 128), F32),
            pltpu.VMEM((2, 2 * ROWS, 256), BF16),
            pltpu.VMEM((4, 4, 2 * ROWS, 256), BF16),
            pltpu.VMEM((8, 128, WCOLS), BF16),
            pltpu.VMEM((8 * ROWS, WCOLS), F32),
            pltpu.VMEM((4, 2 * ROWS, WCOLS), BF16),
            pltpu.VMEM((4, 2 * ROWS, WCOLS), BF16),
            pltpu.VMEM((2, ROWS, WCOLS), BF16),
            pltpu.VMEM((NP, 2, ROWS, WCOLS), BF16),
            pltpu.VMEM((NP, FB, 128), BF16),
            pltpu.VMEM((NP, 2, ROWS, FB), BF16),
            pltpu.VMEM((NT, TOKENS, FB), BF16),
            pltpu.VMEM((TOKENS, FB), F32),
            pltpu.VMEM((SEQ, SEQ), F32),
            pltpu.VMEM((SEQ, SEQ), F32),
            pltpu.VMEM((NT, SCORED, FB), BF16),
            pltpu.VMEM((NT, half, FB), BF16),
            pltpu.VMEM((4, 2, half, FB), BF16),
            pltpu.VMEM((4, 2, half, FB), BF16),
            pltpu.VMEM((2, half, FB), BF16),
            pltpu.VMEM((half, FB), BF16),
            pltpu.VMEM((4, half // 4, FB), BF16),
            pltpu.VMEM((4, half // 4, FB), BF16),
            pltpu.VMEM((4, half // 4, FB), BF16),
            pltpu.VMEM((half // 4, FB), BF16),
            pltpu.VMEM((2, 4, half // 4, FB), BF16),
            pltpu.VMEM((SEQ, FB), BF16),
            pltpu.VMEM((FB, SCORED), BF16),
            pltpu.VMEM((SEQ, 128), F32),
            pltpu.VMEM((PROMPTS, 8, 128), F32),
            pltpu.VMEM((NT, 8, 128), F32),
            pltpu.VMEM((NT, share, SCORED), BF16),
            pltpu.VMEM((NT, share, SCORED), BF16),
            dma((7,)),
            dma((NT,)), dma((NT,)),
            dma((2, NT)), dma((4, 4)),
            dma((4,)), dma((4,)),
            dma((7,)), dma((8,)),
            dma((N_SENDS,)), dma((NP,)),
            dma((N_SENDS,)), dma((NP,)),
            dma((N_SENDS,)), dma((NP,)),
            dma((32,)), dma((NT, PROMPTS)),
            dma((22,)), dma((11,)), dma((4,)), dma((4,)), dma((4,)),
            dma((NT,)), dma((NT,)), dma((NT,)), dma((NT,)),
        ],
        compiler_params=pltpu.CompilerParams(
            collective_id=0, has_side_effects=True, vmem_limit_bytes=60 * 1024 * 1024
        ),
        cost_estimate=pl.CostEstimate(
            flops=4 * 10**9, bytes_accessed=20 * 2**20, transcendentals=10**6
        ),
        name="layer",
    )(*operands)


def rope_tables():
    half = HD // 2
    exponents = -(np.arange(half, dtype=np.float32) * np.float32(2.0 / HD))
    freqs = (np.float32(THETA) ** exponents).astype(np.float32)
    angles = np.arange(SEQ, dtype=np.float32)[:, None] * freqs[None, :]
    cosine, sine = np.cos(angles), np.sin(angles)
    return (
        np.concatenate([cosine, cosine], axis=1).astype(np.float32),
        np.concatenate([-sine, sine], axis=1).astype(np.float32),
    )


def on_device(
    resid_corrupt, resid_clean, patch_level, patch_mask, norm_gain, final_gain,
    w_query, w_key, w_value, w_out, unembed, scored_ids, base_logits,
):
    cosine, sine = rope_tables()
    out = layer(
        resid_corrupt, resid_clean, w_query, w_key, w_value, w_out, unembed,
        patch_level, patch_mask, scored_ids[None, :], norm_gain, final_gain, jnp.asarray(cosine), jnp.asarray(sine),
    )
    return (out - base_logits)[None]


def solution(mesh):
    placed = (
        P(None, "tp"),
        P(None, "patch", "tp"),
        P("patch"),
        P("patch", None),
        P("tp"),
        P("tp"),
        P("patch", "tp"),
        P("patch", "tp"),
        P("patch", "tp"),
        P("tp", "patch"),
        P(("patch", "tp"), None),
        P(),
        P("tp", None),
    )
    return jax.shard_map(
        on_device, mesh=mesh, in_specs=placed, out_specs=P("patch", "tp", None), check_vma=False
    )
```

```python
import jax
import jax.numpy as jnp
import numpy as np
from jax import lax
from jax.experimental import pallas as pl
from jax.experimental.pallas import tpu as pltpu
from jax.sharding import PartitionSpec as P

D = 4096
HD = 128
SEQ = 128
PROMPTS = 4
TOKENS = PROMPTS * SEQ
SCORED = 256
NP = 32
NT = 8
FB = D // NT
ROWS = TOKENS // NP
QCOLS = 512
KVCOL = 128
WCOLS = QCOLS + 2 * KVCOL
EPSILON = 1e-05
THETA = 500000.0
MESH = pl.DeviceIdType.MESH
F32 = jnp.float32
BF16 = jnp.bfloat16
N_SENDS = 31


class PatchGather:
    def __init__(self, own, buf, send, recv):
        self.own, self.buf, self.send, self.recv = own, buf, send, recv
        me = lax.axis_index("patch")
        self.me = me
        self.x, self.z, self.c = me // 8, (me // 2) % 4, me % 2
        self.way = 1 - 2 * self.c
        self.started = []

    def block(self, dx, dz, other=False):
        c = 1 - self.c if other else self.c
        return ((self.x + dx) % 4) * 8 + ((self.z + dz + 4) % 4) * 2 + c

    def copy(self, src, index, target, slot):
        return pltpu.make_async_remote_copy(
            src_ref=src,
            dst_ref=self.buf.at[index],
            send_sem=self.send.at[slot],
            recv_sem=self.recv.at[index],
            device_id={"patch": target},
            device_id_type=MESH,
        )

    def start(self, src, index, target):
        c = self.copy(src, index, target, len(self.started))
        c.start()
        self.started.append(c)

    def wait(self, index):
        self.copy(self.buf.at[index], index, self.block(1, 0), 0).wait_recv()

    def z_send(self):
        for dz in (self.way, -self.way):
            self.start(self.own, self.me, self.block(0, dz))

    def own_send(self):
        for target in (self.block(1, 0), self.block(3, 0), self.block(0, 0, True)):
            self.start(self.own, self.me, target)

    def z_relay(self):
        b = self.block(0, -self.way)
        self.wait(b)
        self.start(self.buf.at[b], b, self.block(0, self.way))

    def spread(self, b):
        for target in (self.block(1, 0), self.block(3, 0), self.block(0, 0, True)):
            self.start(self.buf.at[b], b, target)

    def z_forward(self, relayed=False):
        if not relayed:
            self.z_relay()
        for k, dz in enumerate((-self.way, self.way, 2)):
            b = self.block(0, dz)
            if k > 0:
                self.wait(b)
            self.spread(b)

    def x_near(self, k, then=None):
        for dx in (3, 1):
            b = self.block(dx, (0, -self.way, self.way, 2)[k])
            self.wait(b)
            if (k in (0, 3)) == (dx == 3):
                self.start(self.buf.at[b], b, self.block(4 - dx, 0))
            self.start(self.buf.at[b], b, self.block(0, 0, True))
            if then is not None:
                then(b)

    def x_forward(self, then=None, first=1):
        for k in range(first, 4):
            self.x_near(k, then)

    def far(self, then=None):
        for dz in (0, -self.way, self.way, 2):
            b = self.block(2, dz)
            self.wait(b)
            self.start(self.buf.at[b], b, self.block(0, 0, True))
            if then is not None:
                then(b)

    def core_wait(self, then=None, steps=(0, 3, 1, 2)):
        for dx in steps:
            for dz in (0, self.way, -self.way, 2):
                b = self.block(dx, dz, True)
                self.wait(b)
                if then is not None:
                    then(b)

    def drain(self):
        for c in self.started:
            c.wait_send()


def layer_kernel(
    corrupt_hbm, clean_hbm, wq_hbm, wk_hbm, wv_hbm, wo_hbm, unembed_hbm,
    level_ref, mask_ref, ids_ref, ngain_ref, fgain_ref, cos_ref, sin_ref,
    out_ref,
    corrupt_ref, clean_ref, wo_ref, wo_own, unembed_ref,
    x_own, x_sum, x_got, nsend, ngot, wbuf, acc, pbuf, pgot, qown, qbuf, obuf, cbuf, att, head, early_ref, late_ref,
    chosen, chosen_got, paired, spread, mine, mine_got, spread_z, sum_z, sum_x, own_x, score, fin, score_t, squares, ssq, ssq_got, lg, lg_got,
    local, x_send, x_recv, v_send, v_recv, p_send, p_recv, w_send, w_recv, q_send, q_recv, o_send, o_recv, c_send, c_recv, a_send, a_recv,
    s_send, s_recv, sz_recv, sx_recv, sg_recv, l_send, l_recv, n_send, n_recv,
):
    t = lax.axis_index("tp")
    q = PatchGather(qown, qbuf, q_send, q_recv)
    o = PatchGather(wo_own, obuf, o_send, o_recv)
    cl = PatchGather(clean_ref, cbuf, c_send, c_recv)
    w = q
    me, px, pz, pc = w.me, w.x, w.z, w.c
    ty, tz = t // 2, t % 2
    beside = t + 1 - 2 * tz
    others = [(t + k) % NT for k in range(1, NT)]
    z_others = [(k, (pz + k) % 4) for k in (1, 3, 2)]
    x_others = [(k, (px + k) % 4) for k in (1, 3, 2)]
    partner = w.block(0, 0, True)
    swap_p, swap_t = 4 * t + me % 4, me // 4
    swaps = swap_t != t

    loads = [
        pltpu.make_async_copy(src, dst, local.at[k])
        for k, (src, dst) in enumerate(
            [
                (corrupt_hbm, corrupt_ref),
                (clean_hbm, clean_ref),
                (wq_hbm, wbuf.at[2 * px + pc, :, pl.ds(0, QCOLS)]),
                (wk_hbm, wbuf.at[2 * px + pc, :, pl.ds(QCOLS, KVCOL)]),
                (wv_hbm, wbuf.at[2 * px + pc, :, pl.ds(QCOLS + KVCOL, KVCOL)]),
                (wo_hbm, wo_ref),
                (unembed_hbm, unembed_ref),
            ]
        )
    ]
    for c in loads:
        c.start()
    barrier = pltpu.get_barrier_semaphore()
    peers = (
        [{"tp": k} for k in others]
        + [{"patch": w.block(0, dz)} for dz in (1, 3, 2)]
        + [{"patch": w.block(dx, 0)} for dx in (1, 3, 2)]
        + [{"patch": partner}]
        + [{"patch": w.block(0, dz), "tp": k} for dz in (1, 3, 2) for k in others]
    )
    for peer in peers:
        pl.semaphore_signal(barrier, inc=1, device_id=peer, device_id_type=MESH)

    @pl.when(swaps)
    def _():
        pl.semaphore_signal(
            barrier, inc=1, device_id={"patch": swap_p, "tp": swap_t}, device_id_type=MESH
        )

    for c in loads[:2]:
        c.wait()
    x_own[:ROWS] = corrupt_ref[pl.ds(pl.multiple_of(me * ROWS, ROWS), ROWS), :].astype(F32)
    x_own[ROWS:] = clean_ref[0].astype(F32)
    v = x_own[...]
    x_sum[...] = jnp.broadcast_to(jnp.sum(v * v, axis=1, keepdims=True), (2 * ROWS, 128))
    spliced = jnp.transpose(jnp.broadcast_to(mask_ref[...].astype(F32), (SEQ, SEQ)))
    level = level_ref[0].astype(F32)
    early_ref[...] = spliced * (1.0 - level)
    late_ref[...] = spliced * level
    cbuf[me] = clean_ref[...]
    for c in loads[2:6]:
        c.wait()
    pl.semaphore_wait(barrier, len(peers) + swaps.astype(jnp.int32))

    started = []

    def begin(c):
        c.start()
        started.append(c)

    def x_copy(k, target, to):
        return pltpu.make_async_remote_copy(
            src_ref=x_sum, dst_ref=x_got.at[to], send_sem=x_send.at[k], recv_sem=x_recv.at[to],
            device_id={"tp": target}, device_id_type=MESH,
        )

    def v_copy(h, k, x, z, where):
        return pltpu.make_async_remote_copy(
            src_ref=nsend.at[h], dst_ref=ngot.at[x, z], send_sem=v_send.at[h, k], recv_sem=v_recv.at[x, z],
            device_id=where, device_id_type=MESH,
        )

    def p_copy(k, source, to):
        return pltpu.make_async_remote_copy(
            src_ref=pbuf.at[source], dst_ref=pgot.at[to], send_sem=p_send.at[k], recv_sem=p_recv.at[to],
            device_id={"patch": w.block(0, k)}, device_id_type=MESH,
        )

    def w_copy(slot, dx, c, target):
        index = 2 * ((px + dx + 4) % 4) + c
        return pltpu.make_async_remote_copy(
            src_ref=wbuf.at[index], dst_ref=wbuf.at[index], send_sem=w_send.at[slot], recv_sem=w_recv.at[index],
            device_id={"patch": target}, device_id_type=MESH,
        )

    def s_copy(src, dst, send, recv, where):
        return pltpu.make_async_remote_copy(
            src_ref=src, dst_ref=dst, send_sem=s_send.at[send], recv_sem=recv,
            device_id=where, device_id_type=MESH,
        )

    for k, target in enumerate(others):
        begin(x_copy(k, target, t))
    begin(w_copy(0, 0, pc, w.block(1, 0)))
    begin(w_copy(1, 0, pc, w.block(3, 0)))
    begin(w_copy(2, 0, pc, partner))
    swap = s_copy(wo_ref, wo_own, 21, s_recv.at[10], {"patch": swap_p, "tp": swap_t})

    @pl.when(swaps)
    def _():
        swap.start()

    loads[6].wait()
    rows_dev = unembed_ref.shape[0]
    wanted = jnp.transpose(jnp.broadcast_to(ids_ref[...].astype(F32), (SCORED, SCORED)))[:, :1]
    wanted = wanted.astype(jnp.int32) - (me * NT + t) * rows_dev
    owned = jnp.where(
        wanted == lax.broadcasted_iota(jnp.int32, (SCORED, rows_dev), 1), 1.0, 0.0
    ).astype(BF16)
    for k in range(NT):
        chosen[k] = jnp.dot(
            owned, unembed_ref[:, FB * k : FB * (k + 1)], preferred_element_type=F32
        ).astype(BF16)
    half = SCORED // 2
    pair = s_copy(
        chosen.at[:, pl.ds(pl.multiple_of(half * (1 - pc), half), half)],
        chosen_got, 0, s_recv.at[0], {"patch": partner},
    )
    begin(pair)

    total = x_sum[...]
    for target in others:
        x_copy(0, target, target).wait_recv()
        total = total + x_got[target]
    scale = lax.rsqrt(total[:, :1] / D + EPSILON)
    v = (x_own[...] * scale * ngain_ref[...].astype(F32).reshape(1, FB)).astype(BF16)
    halves = []
    for h in range(2):
        nsend[h] = v[:, 256 * h : 256 * (h + 1)]
    for h in range(2):
        z_to = 2 * tz + h
        for k in range(NT):
            c = v_copy(h, k, ty, pz, {"patch": 8 * px + 2 * z_to + pc, "tp": (t + k) % NT})
            if k > 0:
                begin(c)
            else:
                halves.append((z_to, c))

                @pl.when(z_to != pz)
                def _(c=c):
                    c.start()

    @pl.when(pz // 2 == tz)
    def _():
        ngot[ty, pz] = nsend[pz % 2]

    w_copy(0, -w.way, pc, partner).wait_recv()
    begin(w_copy(3, -w.way, pc, w.block(w.way, 0)))
    begin(w_copy(4, -w.way, pc, partner))
    w_copy(0, w.way, pc, partner).wait_recv()
    begin(w_copy(5, w.way, pc, partner))

    @pl.when(swaps)
    def _():
        swap.wait_recv()

    @pl.when(jnp.logical_not(swaps))
    def _():
        wo_own[...] = wo_ref[...]

    o.z_send()
    pair.wait_recv()
    paired[...] = (
        chosen[:, pl.ds(pl.multiple_of(half * pc, half), half)] + chosen_got[...]
    ).reshape(4, 2, half, FB)
    y_others = [(k, (ty + k) % 4) for k in (1, 3, 2)]
    for k, y in y_others:
        begin(s_copy(paired.at[y], spread.at[ty], k, s_recv.at[1 + ty], {"tp": 2 * y + tz}))

    w_copy(0, 2, pc, partner).wait_recv()
    begin(w_copy(6, 2, pc, partner))
    for kz in range(4):
        z_from = (pz + kz) % 4
        for x in range(4):
            t_from = 2 * x + pz // 2
            c = v_copy(0, 0, x, z_from, {"patch": partner})
            if kz > 0:
                c.wait_recv()
            else:

                @pl.when(t_from != t)
                def _(c=c):
                    c.wait_recv()

    for dx in range(4):
        w_copy(0, dx, 1 - pc, partner).wait_recv()
    for x in range(4):
        piece = jnp.dot(
            ngot[x].reshape(8 * ROWS, 256), wbuf[2 * x : 2 * x + 2].reshape(256, WCOLS),
            preferred_element_type=F32,
        )
        if x == 0:
            acc[...] = piece
        else:
            acc[...] += piece
    pbuf[...] = acc[...].astype(BF16).reshape(4, 2 * ROWS, WCOLS)
    for k, target in z_others:
        begin(p_copy(k, target, pz))
    o.z_relay()
    o.own_send()
    obuf[me] = wo_own[...]


    full = acc[pl.ds(pl.multiple_of(2 * ROWS * pz, 2 * ROWS), 2 * ROWS), :]
    for k, target in z_others:
        p_copy(k, target, target).wait_recv()
        full = full + pgot[target].astype(F32)

    at = pl.ds(pl.multiple_of((me * ROWS) % SEQ, ROWS), ROWS)
    cosine = jnp.concatenate([cos_ref[at, :]] * 2, axis=0)
    sine = jnp.concatenate([sin_ref[at, :]] * 2, axis=0)
    for h in range(WCOLS // HD):
        v = full[:, HD * h : HD * (h + 1)]
        if h < 5:
            v = v * cosine + pltpu.roll(v, HD // 2, 1) * sine
        v = v.astype(BF16)
        for s in range(2):
            qown[s, :, HD * h : HD * (h + 1)] = v[ROWS * s : ROWS * (s + 1)]
    qbuf[me] = qown[...]
    q.z_send()
    q.own_send()
    cl.z_send()
    v = paired[ty]
    for k, y in y_others:
        s_copy(paired.at[y], spread.at[y], 0, s_recv.at[1 + y], {"tp": 2 * y + tz}).wait_recv()
        v = v + spread[y]
    mine[...] = v
    begin(s_copy(mine.at[1 - tz], mine_got, 4, s_recv.at[5], {"tp": beside}))
    o.z_forward(True)

    early = early_ref[...] > 0.5
    row = lax.broadcasted_iota(jnp.int32, (4 * SEQ, SEQ), 0) % SEQ
    col = lax.broadcasted_iota(jnp.int32, (4 * SEQ, SEQ), 1)
    causal = row >= col

    def a_copy(index, n, source, target):
        rows = pl.ds(SEQ * n, SEQ)
        return pltpu.make_async_remote_copy(
            src_ref=att.at[source, rows], dst_ref=att.at[source, rows],
            send_sem=a_send.at[index], recv_sem=a_recv.at[source, n],
            device_id={"tp": target}, device_id_type=MESH,
        )

    a_count = []

    def a_start(n, source, target):
        begin(a_copy(len(a_count), n, source, target))
        a_count.append(n)

    def a_wait(n, source):
        a_copy(0, n, source, others[0]).wait_recv()

    up, down, far_y = ((ty + 1) % 4) * 2, ((ty + 3) % 4) * 2, ((ty + 2) % 4) * 2
    near = (down, up)

    def across(n):
        return n < 2

    def clockwise(n):
        return n % 2 == 0

    def first(n):
        for y in near:
            a_wait(n, y + tz)
            if clockwise(n) == (y is down):
                a_start(n, y + tz, (up if y is down else down) + tz)
            if across(n):
                a_start(n, y + tz, beside)
        a_wait(n, beside)
        if not across(n):
            a_start(n, beside, up + tz)
            a_start(n, beside, down + tz)

    def second(n):
        a_wait(n, far_y + tz)
        if across(n):
            a_start(n, far_y + tz, beside)

    def crossed(n):
        for y in near:
            a_wait(n, y + 1 - tz)
            if not across(n) and clockwise(n) == (y is down):
                a_start(n, y + 1 - tz, (up if y is down else down) + tz)

    def third(n):
        a_wait(n, far_y + 1 - tz)

    prompts = [(px + dx) % 4 for dx in (0, 3, 1, 2)]

    def attend(n):
        prompt = prompts[n]

        def picked(lo, hi):
            a = qbuf[pl.ds(8 * prompt, 8), 0, :, lo:hi].reshape(SEQ, hi - lo).astype(F32)
            b = qbuf[pl.ds(8 * prompt, 8), 1, :, lo:hi].reshape(SEQ, hi - lo).astype(F32)
            return jnp.where(early, b, a).astype(BF16)

        queries = jnp.concatenate([picked(HD * h, HD * (h + 1)) for h in range(4)], axis=0)
        keys = picked(QCOLS, QCOLS + HD)
        values = picked(QCOLS + HD, QCOLS + 2 * HD)
        scores = lax.dot_general(
            queries, keys, (((1,), (1,)), ((), ())), preferred_element_type=F32
        ) * HD ** (-0.5)
        scores = jnp.where(causal, scores, -1e30)
        scores = jnp.exp(scores - jnp.max(scores, axis=1, keepdims=True))
        probs = (scores / jnp.sum(scores, axis=1, keepdims=True)).astype(BF16)
        heads = jnp.dot(probs, values, preferred_element_type=F32).astype(BF16)
        for h in range(4):
            att[t, SEQ * n : SEQ * (n + 1), HD * h : HD * (h + 1)] = heads[SEQ * h : SEQ * (h + 1)]
        for target in (up + tz, down + tz, beside):
            a_start(n, t, target)

    q.z_forward()
    q.x_near(0)
    q.core_wait(steps=(0,))
    attend(0)

    s_copy(mine.at[1 - tz], mine_got, 4, s_recv.at[5], {"tp": beside}).wait_recv()
    spread_z[...] = (mine[tz] + mine_got[...]).reshape(4, half // 4, FB)
    for k, target in z_others:
        begin(s_copy(spread_z.at[target], sum_z.at[pz], 8 + k, sz_recv.at[pz], {"patch": w.block(0, k)}))

    cl.z_relay()
    q.x_forward()
    o.x_near(0)
    q.core_wait(steps=(3, 1))
    attend(1)
    attend(2)

    v = spread_z[pz]
    for k, target in z_others:
        s_copy(spread_z.at[target], sum_z.at[target], 0, sz_recv.at[target], {"patch": w.block(0, k)}).wait_recv()
        v = v + sum_z[target]
    own_x[...] = v
    for k, target in x_others:
        begin(s_copy(own_x, sum_x.at[px], 12 + k, sx_recv.at[px], {"patch": w.block(k, 0)}))

    first(0)
    cl.own_send()
    cl.z_forward(True)
    q.far()
    q.core_wait(steps=(2,))
    attend(3)
    o.x_near(1)

    v = own_x[...]
    for k, target in x_others:
        s_copy(own_x, sum_x.at[target], 0, sx_recv.at[target], {"patch": w.block(k, 0)}).wait_recv()
        v = v + sum_x[target]
    score[pc, pz] = v
    for k, target in z_others:
        begin(s_copy(score.at[pc, pz], score.at[pc, pz], 16 + k, sg_recv.at[pz], {"patch": w.block(0, k)}))

    last = far_y + 1 - tz

    def project(n, count, sources, fresh=False):
        rows = pl.ds(SEQ * n, SEQ * count)
        for k, source in enumerate(sources):
            block = jnp.concatenate([obuf[4 * source + j] for j in range(4)], axis=1)
            piece = jnp.dot(att[source, rows], block, preferred_element_type=F32)
            if fresh and k == 0:
                head[rows] = piece
            else:
                head[rows] += piece

    first(1)
    first(2)
    second(0)

    o.x_near(2)
    o.x_near(3)
    first(3)
    second(1)
    crossed(2)
    cl.x_forward(first=0)

    o.far()
    crossed(3)
    for k, target in z_others:
        s_copy(score.at[pc, target], score.at[pc, target], 0, sg_recv.at[target], {"patch": w.block(0, k)}).wait_recv()
    begin(s_copy(score.at[pc], score.at[pc], 20, s_recv.at[9], {"patch": partner}))
    o.core_wait()
    project(0, 4, (t, beside, up + tz, down + tz), True)
    cl.far()
    crossed(0)
    crossed(1)
    second(2)
    second(3)
    project(0, 4, (far_y + tz, up + 1 - tz, down + 1 - tz))
    s_copy(score.at[pc], score.at[1 - pc], 0, s_recv.at[9], {"patch": partner}).wait_recv()
    score_t[...] = jnp.transpose(score[...].reshape(SCORED, FB).astype(F32)).astype(BF16)
    cl.core_wait()

    gain = fgain_ref[...].astype(F32).reshape(1, FB)
    share = TOKENS // NT

    def l_copy(target, to):
        return pltpu.make_async_remote_copy(
            src_ref=lg.at[target], dst_ref=lg_got.at[to], send_sem=l_send.at[target], recv_sem=l_recv.at[to],
            device_id={"tp": target}, device_id_type=MESH,
        )

    def n_copy(target, to):
        return pltpu.make_async_remote_copy(
            src_ref=ssq.at[target // 2], dst_ref=ssq_got.at[to], send_sem=n_send.at[target], recv_sem=n_recv.at[to],
            device_id={"tp": target}, device_id_type=MESH,
        )

    for n in (2, 3, 0, 1):
        if n == 0:
            third(0)
            third(1)
            project(0, 2, (last,))
        if n == 2:
            third(2)
            third(3)
            project(2, 2, (last,))

        def finish(i, carry, n=n):
            at = pl.ds(pl.multiple_of(SEQ * n + ROWS * i, ROWS), ROWS)
            token = pl.ds(pl.multiple_of(SEQ * prompts[n] + ROWS * i, ROWS), ROWS)
            local_at = pl.ds(pl.multiple_of(ROWS * i, ROWS), ROWS)
            e = early_ref[local_at, :1] > 0.5
            late = late_ref[local_at, :1] > 0.5
            v = corrupt_ref[token, :].astype(F32)
            v = jnp.where(e, cbuf[8 * prompts[n] + i, 0].astype(F32), v)
            v = v + head[at, :]
            v = jnp.where(late, cbuf[8 * prompts[n] + i, 1].astype(F32), v)
            squares[local_at, :] = jnp.broadcast_to(
                jnp.sum(v * v, axis=1, keepdims=True), (ROWS, 128)
            )
            fin[local_at, :] = (v * gain).astype(BF16)
            return carry

        lax.fori_loop(0, SEQ // ROWS, finish, 0, unroll=4)
        ssq[prompts[n]] = jnp.transpose(squares[...])[:8]
        value = jnp.dot(fin[...], score_t[...], preferred_element_type=F32).astype(BF16)
        for s in range(2):
            target = 2 * prompts[n] + s
            lg[target] = value[share * s : share * (s + 1)]

            @pl.when(target != t)
            def _(target=target):
                n_copy(target, t).start()
                l_copy(target, t).start()

    logits = lg[t].astype(F32)
    total = ssq[ty]
    for target in others:
        n_copy(target, target).wait_recv()
        l_copy(target, target).wait_recv()
        logits = logits + lg_got[target].astype(F32)
        total = total + ssq_got[target]
    scale = jnp.transpose(jnp.broadcast_to(lax.rsqrt(total[:1] / D + EPSILON), (SEQ, SEQ)))
    scale = jnp.where(tz == 0, scale[:share], scale[share:])
    out_ref[...] = logits * scale[:, :1]

    for target in others:
        n_copy(target, t).wait_send()
        l_copy(target, t).wait_send()

    @pl.when(swaps)
    def _():
        swap.wait_send()

    for z_to, c in halves:

        @pl.when(z_to != pz)
        def _(c=c):
            c.wait_send()

    for c in started:
        c.wait_send()
    for g in (q, o, cl):
        g.drain()


def layer(*operands):
    vmem = pl.BlockSpec(memory_space=pltpu.VMEM)
    smem = pl.BlockSpec(memory_space=pltpu.SMEM)
    hbm = pl.BlockSpec(memory_space=pl.ANY)
    dma = pltpu.SemaphoreType.DMA
    share = TOKENS // NT
    half = SCORED // 2
    rows_dev = operands[6].shape[0]
    return pl.pallas_call(
        layer_kernel,
        out_shape=jax.ShapeDtypeStruct((share, SCORED), F32),
        in_specs=[hbm] * 7 + [smem] + [vmem] * 6,
        out_specs=vmem,
        scratch_shapes=[
            pltpu.VMEM((TOKENS, FB), BF16),
            pltpu.VMEM((2, ROWS, FB), BF16),
            pltpu.VMEM((FB, 128), BF16),
            pltpu.VMEM((FB, 128), BF16),
            pltpu.VMEM((rows_dev, D), BF16),
            pltpu.VMEM((2 * ROWS, FB), F32),
            pltpu.VMEM((2 * ROWS, 128), F32),
            pltpu.VMEM((NT, 2 * ROWS, 128), F32),
            pltpu.VMEM((2, 2 * ROWS, 256), BF16),
            pltpu.VMEM((4, 4, 2 * ROWS, 256), BF16),
            pltpu.VMEM((8, 128, WCOLS), BF16),
            pltpu.VMEM((8 * ROWS, WCOLS), F32),
            pltpu.VMEM((4, 2 * ROWS, WCOLS), BF16),
            pltpu.VMEM((4, 2 * ROWS, WCOLS), BF16),
            pltpu.VMEM((2, ROWS, WCOLS), BF16),
            pltpu.VMEM((NP, 2, ROWS, WCOLS), BF16),
            pltpu.VMEM((NP, FB, 128), BF16),
            pltpu.VMEM((NP, 2, ROWS, FB), BF16),
            pltpu.VMEM((NT, TOKENS, FB), BF16),
            pltpu.VMEM((TOKENS, FB), F32),
            pltpu.VMEM((SEQ, SEQ), F32),
            pltpu.VMEM((SEQ, SEQ), F32),
            pltpu.VMEM((NT, SCORED, FB), BF16),
            pltpu.VMEM((NT, half, FB), BF16),
            pltpu.VMEM((4, 2, half, FB), BF16),
            pltpu.VMEM((4, 2, half, FB), BF16),
            pltpu.VMEM((2, half, FB), BF16),
            pltpu.VMEM((half, FB), BF16),
            pltpu.VMEM((4, half // 4, FB), BF16),
            pltpu.VMEM((4, half // 4, FB), BF16),
            pltpu.VMEM((4, half // 4, FB), BF16),
            pltpu.VMEM((half // 4, FB), BF16),
            pltpu.VMEM((2, 4, half // 4, FB), BF16),
            pltpu.VMEM((SEQ, FB), BF16),
            pltpu.VMEM((FB, SCORED), BF16),
            pltpu.VMEM((SEQ, 128), F32),
            pltpu.VMEM((PROMPTS, 8, 128), F32),
            pltpu.VMEM((NT, 8, 128), F32),
            pltpu.VMEM((NT, share, SCORED), BF16),
            pltpu.VMEM((NT, share, SCORED), BF16),
            dma((7,)),
            dma((NT,)), dma((NT,)),
            dma((2, NT)), dma((4, 4)),
            dma((4,)), dma((4,)),
            dma((7,)), dma((8,)),
            dma((N_SENDS,)), dma((NP,)),
            dma((N_SENDS,)), dma((NP,)),
            dma((N_SENDS,)), dma((NP,)),
            dma((32,)), dma((NT, PROMPTS)),
            dma((22,)), dma((11,)), dma((4,)), dma((4,)), dma((4,)),
            dma((NT,)), dma((NT,)), dma((NT,)), dma((NT,)),
        ],
        compiler_params=pltpu.CompilerParams(
            collective_id=0, has_side_effects=True, vmem_limit_bytes=60 * 1024 * 1024
        ),
        cost_estimate=pl.CostEstimate(
            flops=4 * 10**9, bytes_accessed=20 * 2**20, transcendentals=10**6
        ),
        name="layer",
    )(*operands)


def rope_tables():
    half = HD // 2
    exponents = -(np.arange(half, dtype=np.float32) * np.float32(2.0 / HD))
    freqs = (np.float32(THETA) ** exponents).astype(np.float32)
    angles = np.arange(SEQ, dtype=np.float32)[:, None] * freqs[None, :]
    cosine, sine = np.cos(angles), np.sin(angles)
    return (
        np.concatenate([cosine, cosine], axis=1).astype(np.float32),
        np.concatenate([-sine, sine], axis=1).astype(np.float32),
    )


def on_device(
    resid_corrupt, resid_clean, patch_level, patch_mask, norm_gain, final_gain,
    w_query, w_key, w_value, w_out, unembed, scored_ids, base_logits,
):
    cosine, sine = rope_tables()
    out = layer(
        resid_corrupt, resid_clean, w_query, w_key, w_value, w_out, unembed,
        patch_level, patch_mask, scored_ids[None, :], norm_gain, final_gain, jnp.asarray(cosine), jnp.asarray(sine),
    )
    return (out - base_logits)[None]


def solution(mesh):
    placed = (
        P(None, "tp"),
        P(None, "patch", "tp"),
        P("patch"),
        P("patch", None),
        P("tp"),
        P("tp"),
        P("patch", "tp"),
        P("patch", "tp"),
        P("patch", "tp"),
        P("tp", "patch"),
        P(("patch", "tp"), None),
        P(),
        P("tp", None),
    )
    return jax.shard_map(
        on_device, mesh=mesh, in_specs=placed, out_specs=P("patch", "tp", None), check_vma=False
    )
```
